1024 devices in a mesh: dp: 8 (over y), seq: 8 (over x, core), tp: 16 (over z).
Axes of the slice: x: 4, y: 8, z: 16, core: 2. Of those that a mesh axis runs over, the one named last changes fastest.
Arguments:
- tokens: bfloat16 [16384, 4096], P(('dp', 'seq', 'tp')), parts along dimension 0, may hold values from -6 to 6
- pre_gain: float32 [4096], replicated, may hold values from 0.25 to 1.75
- proj_inner: bfloat16 [4096, 4096], P(None, 'tp'), may hold values from -0.09375 to 0.09375
- proj_gate: bfloat16 [4096, 4096], P(None, 'tp'), may hold values from -0.09375 to 0.09375
- proj_states: bfloat16 [4096, 1024], P(None, 'tp'), may hold values from -0.09375 to 0.09375
- proj_step: bfloat16 [4096, 64], P(None, 'tp'), may hold values from -0.09375 to 0.09375
- step_bias: float32 [64], P('tp'), may hold values from -5 to -3
- log_rate: float32 [64], P('tp'), as said below
- conv_inner: float32 [4, 4096], P(None, 'tp'), may hold values from -3 to 3
- conv_states: float32 [4, 1024], P(None, 'tp'), may hold values from -3 to 3
- skip_gain: float32 [64], P('tp'), may hold values from 1 to 4
- norm_gain: float32 [4096], P('tp'), may hold values from 0.25 to 1.75
- proj_output: bfloat16 [4096, 4096], P('tp'), may hold values from -0.09375 to 0.09375
Outputs:
- layer_out: bfloat16 [16384, 4096], P(('dp', 'seq', 'tp')), parts along dimension 0
The draws below stay inside these ranges and needn't reach their ends.
There are 8 independent parts, one for each index of `dp`. The reference program is written for one: setup_inputs(seed, part) draws one part's arguments, and reference() takes and returns one part's arrays. A program takes and returns all parts, laid end to end along the dimension named above; an argument that names none is the same for every part. Nothing has to cross between parts.
Inputs may be any that keep to these rules, and one draw needn't show every extreme that they name: exp(log_rate) lies between 0.1 / (0.035 * 2048) and 1 / (25 * 0.035).
All inputs are finite; a program needn't handle non-finite values.
Results may differ from the reference program's by a relative error of at most 0.017.
Values may be sent and summed in bfloat16 or wider, within the bound.
No kernel may reach another device: no remote copies, remote signals or barrier semaphores. Data moves between devices by JAX's collectives and lax.ppermute only.
A program may use at most 64 MiB of HBM per device.

```python
from functools import partial
import jax
import jax.numpy as jnp
from jax import lax

D = 4096
HEADS = 64
HEAD_DIM = 64
STATE = 128
KERNEL = 4
BLOCK = 128
INNER = 4096
GROUPS = 4
SEQ_LEN = 2048


def draw_log_rate(key, part):
    picked = jax.random.fold_in(key, 11)
    kind_key, slow_key, fast_key = jax.random.split(picked, 3)
    shares = jax.random.uniform(kind_key, (HEADS,), jnp.float32)
    slow_rate = jax.random.uniform(slow_key, (HEADS,), jnp.float32, jnp.log(0.1), jnp.log(1.0)) - jnp.log(0.035 * SEQ_LEN)
    fast_rate = jax.random.uniform(fast_key, (HEADS,), jnp.float32, jnp.log(1.0 / 40.0), jnp.log(1.0 / 25.0)) - jnp.log(0.035)
    limit = 0.5
    return jnp.where(shares < limit, slow_rate, fast_rate)


def steps_of(stream_key, dims, shards, low, high):
    def one(dim, shards_of):
        steps = jax.random.uniform(jax.random.fold_in(jax.random.fold_in(stream_key, 6), dim), (shards_of,), jnp.float32, low / len(shards), high / len(shards))
        return jnp.repeat(jnp.exp(steps), dims[dim] // shards_of).reshape((-1,) + (1,) * (len(dims) - dim - 1))

    gain = one(*shards[0])
    for cut in shards[1:]:
        gain = gain * one(*cut)
    return gain


def bell_draw(rng, dims, deviation, most, cuts=(), held_as=jnp.bfloat16):
    gain = steps_of(rng, dims, cuts, -0.22, 0.18) if cuts else 1.0
    array = jax.random.normal(rng, dims, jnp.float32) * deviation * gain
    return jnp.minimum(jnp.maximum(array, -most), most).astype(held_as)


def setup_inputs(seed: int = 0, part: int = 0) -> dict:
    key_list = jax.random.split(jax.random.key(seed), 14)
    part_keys = jax.random.split(jax.random.fold_in(key_list[13], part), 14)
    return {
        "tokens": bell_draw(part_keys[0], (SEQ_LEN, D), 1.0, 6.0, ((0, 128),)),
        "pre_gain": jnp.clip(1.0 + 0.15 * jax.random.normal(key_list[1], (D,), jnp.float32), 0.25, 1.75),
        "proj_inner": bell_draw(key_list[2], (D, INNER), D ** -0.5, 0.09375, ((1, 16),)),
        "proj_gate": bell_draw(key_list[3], (D, INNER), D ** -0.5, 0.09375, ((1, 16),)),
        "proj_states": bell_draw(key_list[4], (D, 2 * GROUPS * STATE), D ** -0.5, 0.09375, ((1, 16),)),
        "proj_step": bell_draw(key_list[5], (D, HEADS), D ** -0.5, 0.09375, ((1, 16),)),
        "step_bias": jnp.clip(-5.0 + 2.0 * jax.random.uniform(key_list[6], (HEADS,), jnp.float32) ** steps_of(key_list[6], (HEADS,), ((0, 16),), -0.2, 0.2), -5.0, -3.0),
        "log_rate": draw_log_rate(jax.random.fold_in(key_list[13], 71), part),
        "conv_inner": bell_draw(key_list[8], (KERNEL, INNER), KERNEL ** -0.5, 3.0, ((1, 16),), jnp.float32),
        "conv_states": bell_draw(key_list[9], (KERNEL, 2 * GROUPS * STATE), KERNEL ** -0.5, 3.0, ((1, 16),), jnp.float32),
        "skip_gain": jnp.clip(1.0 + 3.0 * jax.random.uniform(key_list[10], (HEADS,), jnp.float32) ** steps_of(key_list[10], (HEADS,), ((0, 16),), -0.2, 0.2), 1.0, 4.0),
        "norm_gain": jnp.clip(1.0 + 0.15 * jax.random.normal(key_list[11], (INNER,), jnp.float32), 0.25, 1.75),
        "proj_output": bell_draw(key_list[12], (INNER, D), INNER ** -0.5, 0.09375, ((0, 16),)),
    }


epsilon = 1e-05
highest = lax.Precision.HIGHEST

def causal_conv(values, kernel_taps, before):
    length = values.shape[0]
    padded = jnp.concatenate((before, values), axis=0)
    running_sum = jnp.zeros(values.shape, jnp.float32)
    for offset in range(kernel_taps.shape[0]):
        running_sum = running_sum + kernel_taps[offset] * padded[offset:offset + length]
    return running_sum

def block_step(carry_state, inputs, copies):
    values, step_size, log_decay, in_states, out_states = inputs
    block_len = values.shape[0]
    running = jnp.cumsum(log_decay, axis=0)
    scores = jnp.einsum('tgn,sgn->gts', out_states, in_states, precision=highest)
    scores = jnp.tile(scores, (copies, 1, 1))
    places = jnp.arange(block_len)
    lower_mask = (places[:, None] >= places[None, :])[None]
    spread = running.T[:, :, None] - running.T[:, None, :]
    decay_table = jnp.where(lower_mask, jnp.exp(jnp.where(lower_mask, spread, 0.0)), 0.0)
    weights = scores * decay_table * step_size.T[:, None, :]
    within = jnp.einsum('hts,shp->thp', weights, values, precision=highest)
    out_heads = jnp.tile(out_states, (1, copies, 1))
    in_heads = jnp.tile(in_states, (1, copies, 1))
    carried = jnp.einsum('thn,hpn->thp', out_heads, carry_state, precision=highest) * jnp.exp(running)[:, :, None]
    tail_decay = jnp.exp(running[-1][None, :] - running) * step_size
    scaled = values * tail_decay[:, :, None]
    new_state = jnp.exp(running[-1])[:, None, None] * carry_state + jnp.einsum('shp,shn->hpn', scaled, in_heads, precision=highest)
    return (new_state, within + carried)

def scan_blocks(values, step_size, log_decay, in_states, out_states, carry_state, block_len, copies):
    row_count, head_count, head_dim = values.shape
    block_count = row_count // block_len

    def split_blocks(source):
        return source.reshape((block_count, block_len) + source.shape[1:])
    final_state, outputs = lax.scan(partial(block_step, copies=copies), carry_state, (split_blocks(values), split_blocks(step_size), split_blocks(log_decay), split_blocks(in_states), split_blocks(out_states)))
    return (final_state, outputs.reshape(row_count, head_count, head_dim))

def reference(tokens, pre_gain, proj_inner, proj_gate, proj_states, proj_step, step_bias, log_rate, conv_inner, conv_states, skip_gain, norm_gain, proj_output):
    tokens_wide = tokens.astype(jnp.float32)
    normed = (tokens_wide * lax.rsqrt(lax.optimization_barrier(jnp.mean(tokens_wide * tokens_wide, axis=1, keepdims=True)) + epsilon) * pre_gain).astype(jnp.bfloat16)
    inner_proj = jnp.dot(normed, proj_inner, preferred_element_type=jnp.float32).astype(jnp.bfloat16)
    gate_proj = jnp.dot(normed, proj_gate, preferred_element_type=jnp.float32).astype(jnp.bfloat16)
    state_proj = jnp.dot(normed, proj_states, preferred_element_type=jnp.float32).astype(jnp.bfloat16)
    step_size = jax.nn.softplus(jnp.dot(normed, proj_step, preferred_element_type=jnp.float32) + step_bias)
    log_decay = -jnp.exp(log_rate) * step_size
    before_inner = jnp.zeros((KERNEL - 1, INNER), jnp.float32)
    before_states = jnp.zeros((KERNEL - 1, 2 * GROUPS * STATE), jnp.float32)
    mixed_inner = jax.nn.silu(causal_conv(inner_proj.astype(jnp.float32), conv_inner, before_inner)).astype(jnp.bfloat16)
    mixed_states = jax.nn.silu(causal_conv(state_proj.astype(jnp.float32), conv_states, before_states)).astype(jnp.bfloat16)
    values = mixed_inner.astype(jnp.float32).reshape(SEQ_LEN, HEADS, HEAD_DIM)
    paired = mixed_states.astype(jnp.float32).reshape(SEQ_LEN, GROUPS, 2, STATE)
    zero_state = jnp.zeros((HEADS, HEAD_DIM, STATE), jnp.float32)
    final_state, scanned = scan_blocks(values, step_size, log_decay, paired[:, :, 0], paired[:, :, 1], zero_state, BLOCK, HEADS // GROUPS)
    ssd_out = scanned + skip_gain[None, :, None] * values
    gated_out = ssd_out * jax.nn.silu(gate_proj.astype(jnp.float32)).reshape(SEQ_LEN, HEADS, HEAD_DIM)
    grouped = gated_out.reshape(SEQ_LEN, HEADS // GROUPS, GROUPS, HEAD_DIM)
    mean_square = lax.optimization_barrier(jnp.mean(grouped * grouped, axis=(1, 3), keepdims=True))
    normal_out = grouped * lax.rsqrt(mean_square + epsilon)
    mixed_out = (normal_out.reshape(SEQ_LEN, INNER) * norm_gain).astype(jnp.bfloat16)
    return (tokens_wide + jnp.dot(mixed_out, proj_output, preferred_element_type=jnp.float32)).astype(jnp.bfloat16)
```

```python
from functools import partial
import math

import jax
import jax.numpy as jnp
from jax import lax
from jax.sharding import PartitionSpec as P

HEAD_DIM = 64
STATE = 128
GROUP_HEADS = 16
BLOCK = 128
GROUPS = 4


epsilon = 1e-05
highest = lax.Precision.HIGHEST


def from_behind(value, axis, steps):
    count = lax.axis_size(axis)
    initial, last = (max(0, -steps), min(count, count - steps))
    return lax.ppermute(value, axis, [(source, source + steps) for source in range(initial, last)])


def in_order(tiles, dim):
    tiles = jnp.moveaxis(tiles, 0, dim)
    dims = tiles.shape
    return tiles.reshape(*dims[:dim], dims[dim] * dims[dim + 1], *dims[dim + 2 :])


def from_everyone(x, axis):
    copies = jnp.broadcast_to(x, (lax.axis_size(axis), *x.shape))
    return lax.all_to_all(copies, axis, split_axis=0, concat_axis=0, tiled=True)


def collect(x, axis, dim):
    return in_order(from_everyone(x, axis), dim)


def sent_together(arrays, axis, dim, along):
    widths = [math.prod(a.shape[along:]) for a in arrays]
    both = jnp.concatenate(
        [a.reshape(*a.shape[:along], w) for a, w in zip(arrays, widths)], axis=along
    )
    out = lax.all_gather(both, axis, axis=dim, tiled=True)
    tiles = jnp.split(out, [sum(widths[:k]) for k in range(1, len(widths))], axis=along)
    return tuple((b.reshape(*out.shape[:along], *a.shape[along:]) for a, b in zip(arrays, tiles)))


def gather_rows(x):
    rows, width = x.shape
    count = lax.axis_size("tp")
    chunk = (2**20 // (2 * rows * count) - 1) // 128 * 128
    whole = width // chunk
    rest = from_everyone(x[:, whole * chunk :], "tp").reshape(count * rows, width - whole * chunk)
    parts = [
        lax.all_gather(x[:, k * chunk : (k + 1) * chunk], "tp", axis=0, tiled=True)
        for k in range(whole)
    ]
    return jnp.concatenate(parts + [rest], axis=1)


def ring_scatter(partial, axis):
    count = lax.axis_size(axis)
    me = lax.axis_index(axis)
    up = [(k, (k + 1) % count) for k in range(count)]
    down = [(k, (k - 1) % count) for k in range(count)]
    far = count // 2
    near = count - 1 - far

    def piece(offset):
        return lax.dynamic_index_in_dim(partial, (me + offset) % count, 0, keepdims=False)

    rising = piece(far)
    falling = piece(-near)
    for step in range(1, far + 1):
        rising = lax.ppermute(rising, axis, up)
        if step <= near:
            falling = lax.ppermute(falling, axis, down)
        if step < far:
            rising = (
                rising.astype(jnp.float32) + piece(far - step).astype(jnp.float32)
            ).astype(partial.dtype)
        if step < near:
            falling = (
                falling.astype(jnp.float32) + piece(step - near).astype(jnp.float32)
            ).astype(partial.dtype)
    return (
        piece(0).astype(jnp.float32) + rising.astype(jnp.float32) + falling.astype(jnp.float32)
    )


def causal_conv(values, kernel_taps, before):
    length = values.shape[0]
    padded = jnp.concatenate((before, values), axis=0)
    running_sum = jnp.zeros(values.shape, jnp.float32)
    for offset in range(kernel_taps.shape[0]):
        running_sum = running_sum + kernel_taps[offset] * padded[offset : offset + length]
    return running_sum


def block_step(carry_state, inputs, copies):
    values, step_size, log_decay, in_states, out_states = inputs
    block_len = values.shape[0]
    running = jnp.cumsum(log_decay, axis=0)
    scores = jnp.einsum("tgn,sgn->gts", out_states, in_states, precision=highest)
    scores = jnp.tile(scores, (copies, 1, 1))
    places = jnp.arange(block_len)
    lower_mask = (places[:, None] >= places[None, :])[None]
    spread = running.T[:, :, None] - running.T[:, None, :]
    decay_table = jnp.where(lower_mask, jnp.exp(jnp.where(lower_mask, spread, 0.0)), 0.0)
    weights = scores * decay_table * step_size.T[:, None, :]
    within = jnp.einsum("hts,shp->thp", weights, values, precision=highest)
    out_heads = jnp.tile(out_states, (1, copies, 1))
    in_heads = jnp.tile(in_states, (1, copies, 1))
    carried = (
        jnp.einsum("thn,hpn->thp", out_heads, carry_state, precision=highest)
        * jnp.exp(running)[:, :, None]
    )
    tail_decay = jnp.exp(running[-1][None, :] - running) * step_size
    scaled = values * tail_decay[:, :, None]
    new_state = jnp.exp(running[-1])[:, None, None] * carry_state + jnp.einsum(
        "shp,shn->hpn", scaled, in_heads, precision=highest
    )
    return (new_state, within + carried)


def scan_blocks(
    values, step_size, log_decay, in_states, out_states, carry_state, block_len, copies
):
    row_count, head_count, head_dim = values.shape
    block_count = row_count // block_len

    def split_blocks(source):
        return source.reshape((block_count, block_len) + source.shape[1:])

    final_state, outputs = lax.scan(
        partial(block_step, copies=copies),
        carry_state,
        (
            split_blocks(values),
            split_blocks(step_size),
            split_blocks(log_decay),
            split_blocks(in_states),
            split_blocks(out_states),
        ),
    )
    return (final_state, outputs.reshape(row_count, head_count, head_dim))


def body(
    tokens,
    pre_gain,
    proj_inner,
    proj_gate,
    proj_states,
    proj_step,
    step_bias,
    log_rate,
    conv_inner,
    conv_states,
    skip_gain,
    norm_gain,
    proj_output,
):
    tokens_wide = tokens.astype(jnp.float32)
    normed = (
        tokens_wide
        * lax.rsqrt(jnp.mean(tokens_wide * tokens_wide, axis=1, keepdims=True) + epsilon)
        * pre_gain
    ).astype(jnp.bfloat16)
    inner_width = proj_inner.shape[1]
    state_width = proj_states.shape[1]
    heads_local = proj_step.shape[1]
    copies = heads_local // GROUPS
    row_piece = gather_rows(normed)
    projected = jnp.concatenate(
        (
            jnp.dot(row_piece, proj_inner, preferred_element_type=jnp.float32),
            jnp.dot(row_piece, proj_gate, preferred_element_type=jnp.float32),
            jnp.dot(row_piece, proj_states, preferred_element_type=jnp.float32),
            jnp.dot(row_piece, proj_step, preferred_element_type=jnp.float32),
        ),
        axis=1,
    )
    row_count = projected.shape[0]
    inner_proj = projected[:, :inner_width].astype(jnp.bfloat16)
    gate_proj = projected[:, inner_width : 2 * inner_width].astype(jnp.bfloat16)
    state_proj = projected[:, 2 * inner_width : 2 * inner_width + state_width].astype(jnp.bfloat16)
    step_size = jax.nn.softplus(projected[:, 2 * inner_width + state_width :] + step_bias)
    log_decay = -jnp.exp(log_rate) * step_size
    margin = conv_inner.shape[0] - 1
    before = from_behind(
        jnp.concatenate((inner_proj[row_count - margin :], state_proj[row_count - margin :]), axis=1),
        "seq",
        1,
    )
    before_inner, before_states = before[:, :inner_width], before[:, inner_width:]
    mixed_inner = jax.nn.silu(
        causal_conv(inner_proj.astype(jnp.float32), conv_inner, before_inner.astype(jnp.float32))
    ).astype(jnp.bfloat16)
    mixed_local = jax.nn.silu(
        causal_conv(state_proj.astype(jnp.float32), conv_states, before_states.astype(jnp.float32))
    ).astype(jnp.bfloat16)
    mixed_all = collect(mixed_local, "tp", 1)
    values = mixed_inner.astype(jnp.float32).reshape(row_count, heads_local, HEAD_DIM)
    paired = mixed_all.astype(jnp.float32).reshape(row_count, GROUPS, 2, STATE)
    in_states = paired[:, :, 0]
    out_states = paired[:, :, 1]
    zero_state = jnp.zeros((heads_local, HEAD_DIM, STATE), jnp.float32)
    final_state, scanned = scan_blocks(
        values, step_size, log_decay, in_states, out_states, zero_state, BLOCK, copies
    )
    decay_sum = jnp.sum(log_decay, axis=0)
    decay_sums, summaries = tuple(
        (
            part.astype(jnp.float32)
            for part in sent_together(
                (decay_sum[None].astype(jnp.bfloat16), final_state[None].astype(jnp.bfloat16)),
                "seq",
                0,
                2,
            )
        )
    )
    position = lax.axis_index("seq")
    device_ids = jnp.arange(decay_sums.shape[0])
    earlier_mask = (device_ids < position)[:, None]
    before_me = jnp.sum(jnp.where(earlier_mask, decay_sums, 0.0), axis=0)
    reach_end = jnp.cumsum(decay_sums, axis=0)
    weights = jnp.where(
        earlier_mask, jnp.exp(jnp.where(earlier_mask, before_me[None] - reach_end, 0.0)), 0.0
    )
    incoming = jnp.einsum("jh,jhpn->hpn", weights, summaries, precision=highest)
    running = jnp.cumsum(log_decay, axis=0)
    out_heads = jnp.tile(out_states, (1, copies, 1))
    carried = (
        jnp.einsum("thn,hpn->thp", out_heads, incoming, precision=highest)
        * jnp.exp(running)[:, :, None]
    )
    ssd_out = scanned + carried + skip_gain[None, :, None] * values
    gated_out = ssd_out * jax.nn.silu(gate_proj.astype(jnp.float32)).reshape(
        row_count, heads_local, HEAD_DIM
    )
    head_squares = jnp.sum(gated_out * gated_out, axis=2)
    every_square = collect(head_squares, "tp", 1)
    group_totals = jnp.sum(
        every_square.reshape(row_count, every_square.shape[1] // GROUPS, GROUPS), axis=1
    )
    mean_square = (group_totals / (GROUP_HEADS * HEAD_DIM))[:, None, :, None]
    grouped = gated_out.reshape(row_count, copies, GROUPS, HEAD_DIM)
    normal_out = grouped * lax.rsqrt(mean_square + epsilon)
    mixed_out = (normal_out.reshape(row_count, inner_width) * norm_gain).astype(jnp.bfloat16)
    partial = jnp.dot(mixed_out, proj_output, preferred_element_type=jnp.float32)
    partial = partial.astype(jnp.bfloat16).reshape(-1, tokens.shape[0], tokens.shape[1])
    summed = ring_scatter(partial, "tp")
    return (tokens_wide + summed).astype(jnp.bfloat16)


def solution(mesh):
    placed = (
        P(("dp", "seq", "tp"), None),
        P(),
        P(None, "tp"),
        P(None, "tp"),
        P(None, "tp"),
        P(None, "tp"),
        P("tp"),
        P("tp"),
        P(None, "tp"),
        P(None, "tp"),
        P("tp"),
        P("tp"),
        P("tp", None),
    )
    return jax.shard_map(
        body, mesh=mesh, in_specs=placed, out_specs=P(("dp", "seq", "tp"), None), check_vma=False
    )
```

```python
import jax
import jax.numpy as jnp
from jax import lax
from jax.experimental import pallas as pl
from jax.experimental.pallas import tpu as pltpu
from jax.sharding import PartitionSpec as P

HEAD_DIM = 64
STATE = 128
GROUP_HEADS = 16
TAPS = 4
TAIL_ROWS = 8
GROUPS = 4


epsilon = 1e-05
highest = lax.Precision.HIGHEST


def from_behind(value, axis, steps):
    count = lax.axis_size(axis)
    initial, last = (max(0, -steps), min(count, count - steps))
    return lax.ppermute(value, axis, [(source, source + steps) for source in range(initial, last)])


def split_dot(exact, wide, dims, exact_first):
    upper = wide.astype(jnp.bfloat16)
    lower = (wide - upper.astype(jnp.float32)).astype(jnp.bfloat16)

    def product(part):
        pair = (exact, part) if exact_first else (part, exact)
        return lax.dot_general(*pair, (dims, ((), ())), preferred_element_type=jnp.float32)

    return product(upper) + product(lower)


def head_lanes(columns, width):
    rows = columns.shape[0]
    return jnp.concatenate(
        [jnp.broadcast_to(columns[:, h : h + 1], (rows, width)) for h in range(GROUPS)], axis=1
    )


def local_scan_kernel(
    inner_ref, halo_ref, taps_ref, states_ref, step_ref, decay_ref, skip_ref,
    local_ref, message_ref, reach_ref, padded,
):
    length = inner_ref.shape[0]
    margin = TAPS - 1
    padded[TAIL_ROWS - margin : TAIL_ROWS, :] = halo_ref[...].astype(jnp.float32)
    padded[TAIL_ROWS:, :] = inner_ref[...].astype(jnp.float32)
    conv = jnp.zeros(inner_ref.shape, jnp.float32)
    for tap in range(TAPS):
        start = TAIL_ROWS - margin + tap
        conv = conv + taps_ref[tap : tap + 1, :] * padded[start : start + length, :]
    mixed = (conv / (1.0 + jnp.exp(-conv))).astype(jnp.bfloat16)
    rows = lax.broadcasted_iota(jnp.int32, (length, length), 0)
    cols = lax.broadcasted_iota(jnp.int32, (length, length), 1)
    lower_mask = rows >= cols
    blank = jnp.zeros((128 - GROUPS, length), jnp.float32)
    step_rows = step_ref[...]
    reach_rows = jnp.dot(
        jnp.concatenate((decay_ref[...], blank), axis=0),
        (rows <= cols).astype(jnp.float32),
        precision=highest,
        preferred_element_type=jnp.float32,
    )
    reach = reach_rows.T
    step = jnp.concatenate((step_rows, blank), axis=0).T
    reach_ref[...] = reach
    final = reach[length - 1 :, :]
    tail = jnp.exp(final - reach) * step
    mixed_wide = mixed.astype(jnp.float32)
    scaled = mixed_wide * head_lanes(tail, HEAD_DIM)
    outs = []
    ends = []
    for g in range(GROUPS):
        low = g * HEAD_DIM
        in_states = states_ref[2 * g * STATE : (2 * g + 1) * STATE, :]
        out_states = states_ref[(2 * g + 1) * STATE : (2 * g + 2) * STATE, :]
        scores = lax.dot_general(
            out_states, in_states, (((0,), (0,)), ((), ())), preferred_element_type=jnp.float32
        )
        spread = jnp.where(lower_mask, reach[:, g : g + 1] - reach_rows[g : g + 1, :], 0.0)
        decay_table = jnp.where(lower_mask, jnp.exp(spread), 0.0)
        weights = scores * decay_table * step_rows[g : g + 1, :]
        outs.append(split_dot(mixed[:, low : low + HEAD_DIM], weights, ((1,), (0,)), False))
        ends.append(split_dot(in_states, scaled[:, low : low + HEAD_DIM], ((1,), (0,)), True))
    local_ref[...] = jnp.concatenate(outs, axis=1) + skip_ref[...] * mixed_wide
    message_ref[0, :STATE, :] = jnp.concatenate(ends, axis=1).astype(jnp.bfloat16)
    total = head_lanes(final, HEAD_DIM)
    upper = total.astype(jnp.bfloat16)
    lower = (total - upper.astype(jnp.float32)).astype(jnp.bfloat16)
    zeros = jnp.zeros((TAIL_ROWS - 1, total.shape[1]), jnp.bfloat16)
    message_ref[0, STATE : STATE + TAIL_ROWS, :] = jnp.concatenate((upper, zeros), axis=0)
    message_ref[0, STATE + TAIL_ROWS :, :] = jnp.concatenate((lower, zeros), axis=0)


def carry_kernel(
    position_ref, messages_ref, states_ref, reach_ref, local_ref, gate_ref, gated_ref, squares_ref
):
    position = position_ref[0]
    width = local_ref.shape[1]
    carry = jnp.zeros((STATE, width), jnp.float32)
    for k in range(messages_ref.shape[0] - 1):
        total = messages_ref[k, STATE : STATE + TAIL_ROWS, :].astype(jnp.float32)
        total = total + messages_ref[k, STATE + TAIL_ROWS :, :].astype(jnp.float32)
        moved = jnp.exp(total[:1, :]) * carry + messages_ref[k, :STATE, :].astype(jnp.float32)
        carry = jnp.where(k < position, moved, carry)
    outs = []
    for g in range(GROUPS):
        low = g * HEAD_DIM
        out_states = states_ref[(2 * g + 1) * STATE : (2 * g + 2) * STATE, :]
        outs.append(split_dot(out_states, carry[:, low : low + HEAD_DIM], ((0,), (0,)), True))
    carried = jnp.concatenate(outs, axis=1) * head_lanes(jnp.exp(reach_ref[...]), HEAD_DIM)
    gate = gate_ref[...].astype(jnp.float32)
    gated = (local_ref[...] + carried) * (gate / (1.0 + jnp.exp(-gate)))
    gated_ref[...] = gated
    owner = lax.broadcasted_iota(jnp.int32, (TAIL_ROWS, width), 1) // HEAD_DIM
    heads = lax.broadcasted_iota(jnp.int32, (TAIL_ROWS, width), 0)
    sums = lax.dot_general(
        (owner == heads).astype(jnp.float32),
        gated * gated,
        (((1,), (1,)), ((), ())),
        precision=highest,
        preferred_element_type=jnp.float32,
    )
    squares_ref[0] = sums[:GROUPS, :]


def in_vmem(count):
    return [pl.BlockSpec(memory_space=pltpu.VMEM)] * count


def local_scan(inner, halo, taps, states, step, decay, skip, interpret=False):
    length, width = inner.shape
    return pl.pallas_call(
        local_scan_kernel,
        out_shape=(
            jax.ShapeDtypeStruct((length, width), jnp.float32),
            jax.ShapeDtypeStruct((1, STATE + 2 * TAIL_ROWS, width), jnp.bfloat16),
            jax.ShapeDtypeStruct((length, 128), jnp.float32),
        ),
        in_specs=in_vmem(7),
        out_specs=tuple(in_vmem(3)),
        scratch_shapes=[pltpu.VMEM((length + TAIL_ROWS, width), jnp.float32)],
        interpret=interpret,
        name="local_scan",
    )(inner, halo, taps, states, step, decay, skip)


def carry_in(position, messages, states, reach, local, gate, interpret=False):
    length, width = local.shape
    return pl.pallas_call(
        carry_kernel,
        out_shape=(
            jax.ShapeDtypeStruct((length, width), jnp.float32),
            jax.ShapeDtypeStruct((1, GROUPS, length), jnp.float32),
        ),
        in_specs=[pl.BlockSpec(memory_space=pltpu.SMEM)] + in_vmem(5),
        out_specs=tuple(in_vmem(2)),
        interpret=interpret,
        name="carry_in",
    )(position, messages, states, reach, local, gate)


def body(
    tokens,
    pre_gain,
    proj_inner,
    proj_gate,
    proj_states,
    proj_step,
    step_bias,
    log_rate,
    conv_inner,
    conv_states,
    skip_gain,
    norm_gain,
    proj_output,
):
    tokens_wide = tokens.astype(jnp.float32)
    normed = (
        tokens_wide
        * lax.rsqrt(jnp.mean(tokens_wide * tokens_wide, axis=1, keepdims=True) + epsilon)
        * pre_gain
    ).astype(jnp.bfloat16)
    inner_width = proj_inner.shape[1]
    state_width = proj_states.shape[1]
    row_piece = lax.all_gather(normed, "tp", axis=0, tiled=True)
    row_count = row_piece.shape[0]
    margin = TAPS - 1

    def project(weight):
        return jnp.dot(row_piece, weight, preferred_element_type=jnp.float32)

    def project_across(weight):
        return lax.dot_general(
            weight, row_piece, (((0,), (1,)), ((), ())), preferred_element_type=jnp.float32
        )

    state_proj = project_across(proj_states).astype(jnp.bfloat16)
    inner_proj = project(proj_inner).astype(jnp.bfloat16)
    gate_proj = project(proj_gate).astype(jnp.bfloat16)
    step_size = jax.nn.softplus(project_across(proj_step) + step_bias[:, None])
    log_decay = -jnp.exp(log_rate)[:, None] * step_size
    before = from_behind(
        jnp.concatenate((inner_proj[row_count - margin :], state_proj[:, row_count - margin :].T), axis=1),
        "seq",
        1,
    )
    before_inner, before_states = before[:, :inner_width], before[:, inner_width:].T
    padded = jnp.concatenate((before_states, state_proj), axis=1).astype(jnp.float32)
    mixed_local = jnp.zeros(state_proj.shape, jnp.float32)
    for tap in range(TAPS):
        mixed_local = mixed_local + conv_states[tap][:, None] * padded[:, tap : tap + row_count]
    mixed_local = jax.nn.silu(mixed_local).astype(jnp.bfloat16)
    mixed_all = lax.all_gather(mixed_local[None], "tp", axis=0, tiled=True)
    mixed_all = mixed_all.reshape(-1, row_count)
    skip_row = jnp.repeat(skip_gain, HEAD_DIM)[None]
    local, message, reach = local_scan(
        inner_proj, before_inner, conv_inner, mixed_all, step_size, log_decay, skip_row
    )
    messages = lax.all_gather(message, "seq", axis=0, tiled=True)
    position = lax.axis_index("seq").astype(jnp.int32).reshape(1)
    gated_out, head_squares = carry_in(position, messages, mixed_all, reach, local, gate_proj)
    every_square = lax.all_gather(head_squares, "tp", axis=0, tiled=True)
    mean_square = jnp.sum(every_square, axis=0) / (GROUP_HEADS * HEAD_DIM)
    scale = jnp.repeat(lax.rsqrt(mean_square + epsilon).T, HEAD_DIM, axis=1)
    mixed_out = (gated_out * scale * norm_gain).astype(jnp.bfloat16)
    summed = lax.psum_scatter(
        jnp.dot(mixed_out, proj_output, preferred_element_type=jnp.float32).astype(jnp.bfloat16),
        "tp",
        scatter_dimension=0,
        tiled=True,
    ).astype(jnp.float32)
    return (tokens_wide + summed).astype(jnp.bfloat16)


def solution(mesh):
    placed = (
        P(("dp", "seq", "tp"), None),
        P(),
        P(None, "tp"),
        P(None, "tp"),
        P(None, "tp"),
        P(None, "tp"),
        P("tp"),
        P("tp"),
        P(None, "tp"),
        P(None, "tp"),
        P("tp"),
        P("tp"),
        P("tp", None),
    )
    return jax.shard_map(
        body, mesh=mesh, in_specs=placed, out_specs=P(("dp", "seq", "tp"), None), check_vma=False
    )
```

```python
import jax
import jax.numpy as jnp
from jax import lax
from jax.experimental import pallas as pl
from jax.experimental.pallas import tpu as pltpu
from jax.sharding import PartitionSpec as P

HEAD_DIM = 64
STATE = 128
GROUP_HEADS = 16
TAPS = 4
TAIL_ROWS = 8
GROUPS = 4


epsilon = 1e-05
highest = lax.Precision.HIGHEST


def from_behind(value, axis, steps):
    count = lax.axis_size(axis)
    initial, last = (max(0, -steps), min(count, count - steps))
    return lax.ppermute(value, axis, [(source, source + steps) for source in range(initial, last)])


def from_everyone(x, axis):
    copies = jnp.broadcast_to(x, (lax.axis_size(axis), *x.shape))
    return lax.all_to_all(copies, axis, split_axis=0, concat_axis=0, tiled=True)


def split_dot(exact, wide, dims, exact_first):
    upper = wide.astype(jnp.bfloat16)
    lower = (wide - upper.astype(jnp.float32)).astype(jnp.bfloat16)

    def product(part):
        pair = (exact, part) if exact_first else (part, exact)
        return lax.dot_general(*pair, (dims, ((), ())), preferred_element_type=jnp.float32)

    return product(upper) + product(lower)


def head_lanes(columns, width):
    rows = columns.shape[0]
    return jnp.concatenate(
        [jnp.broadcast_to(columns[:, h : h + 1], (rows, width)) for h in range(GROUPS)], axis=1
    )


def local_scan_kernel(
    inner_ref, halo_ref, taps_ref, states_ref, step_ref, decay_ref, skip_ref,
    local_ref, message_ref, reach_ref, padded,
):
    length = inner_ref.shape[0]
    margin = TAPS - 1
    padded[TAIL_ROWS - margin : TAIL_ROWS, :] = halo_ref[...].astype(jnp.float32)
    padded[TAIL_ROWS:, :] = inner_ref[...].astype(jnp.float32)
    conv = jnp.zeros(inner_ref.shape, jnp.float32)
    for tap in range(TAPS):
        start = TAIL_ROWS - margin + tap
        conv = conv + taps_ref[tap : tap + 1, :] * padded[start : start + length, :]
    mixed = (conv / (1.0 + jnp.exp(-conv))).astype(jnp.bfloat16)
    rows = lax.broadcasted_iota(jnp.int32, (length, length), 0)
    cols = lax.broadcasted_iota(jnp.int32, (length, length), 1)
    lower_mask = rows >= cols
    blank = jnp.zeros((128 - GROUPS, length), jnp.float32)
    step_rows = step_ref[...]
    reach_rows = jnp.dot(
        jnp.concatenate((decay_ref[...], blank), axis=0),
        (rows <= cols).astype(jnp.float32),
        precision=highest,
        preferred_element_type=jnp.float32,
    )
    reach = reach_rows.T
    step = jnp.concatenate((step_rows, blank), axis=0).T
    reach_ref[...] = reach
    final = reach[length - 1 :, :]
    tail = jnp.exp(final - reach) * step
    mixed_wide = mixed.astype(jnp.float32)
    scaled = mixed_wide * head_lanes(tail, HEAD_DIM)
    outs = []
    ends = []
    for g in range(GROUPS):
        low = g * HEAD_DIM
        in_states = states_ref[2 * g * STATE : (2 * g + 1) * STATE, :]
        out_states = states_ref[(2 * g + 1) * STATE : (2 * g + 2) * STATE, :]
        scores = lax.dot_general(
            out_states, in_states, (((0,), (0,)), ((), ())), preferred_element_type=jnp.float32
        )
        spread = jnp.where(lower_mask, reach[:, g : g + 1] - reach_rows[g : g + 1, :], 0.0)
        decay_table = jnp.where(lower_mask, jnp.exp(spread), 0.0)
        weights = scores * decay_table * step_rows[g : g + 1, :]
        outs.append(split_dot(mixed[:, low : low + HEAD_DIM], weights, ((1,), (0,)), False))
        ends.append(split_dot(in_states, scaled[:, low : low + HEAD_DIM], ((1,), (0,)), True))
    local_ref[...] = jnp.concatenate(outs, axis=1) + skip_ref[...] * mixed_wide
    message_ref[0, :STATE, :] = jnp.concatenate(ends, axis=1).astype(jnp.bfloat16)
    total = head_lanes(final, HEAD_DIM)
    upper = total.astype(jnp.bfloat16)
    lower = (total - upper.astype(jnp.float32)).astype(jnp.bfloat16)
    zeros = jnp.zeros((TAIL_ROWS - 1, total.shape[1]), jnp.bfloat16)
    message_ref[0, STATE : STATE + TAIL_ROWS, :] = jnp.concatenate((upper, zeros), axis=0)
    message_ref[0, STATE + TAIL_ROWS :, :] = jnp.concatenate((lower, zeros), axis=0)


def carry_kernel(
    position_ref, messages_ref, states_ref, reach_ref, local_ref, gate_ref, gated_ref, squares_ref
):
    position = position_ref[0]
    width = local_ref.shape[1]
    carry = jnp.zeros((STATE, width), jnp.float32)
    for k in range(messages_ref.shape[0] - 1):
        total = messages_ref[k, STATE : STATE + TAIL_ROWS, :].astype(jnp.float32)
        total = total + messages_ref[k, STATE + TAIL_ROWS :, :].astype(jnp.float32)
        moved = jnp.exp(total[:1, :]) * carry + messages_ref[k, :STATE, :].astype(jnp.float32)
        carry = jnp.where(k < position, moved, carry)
    outs = []
    for g in range(GROUPS):
        low = g * HEAD_DIM
        out_states = states_ref[(2 * g + 1) * STATE : (2 * g + 2) * STATE, :]
        outs.append(split_dot(out_states, carry[:, low : low + HEAD_DIM], ((0,), (0,)), True))
    carried = jnp.concatenate(outs, axis=1) * head_lanes(jnp.exp(reach_ref[...]), HEAD_DIM)
    gate = gate_ref[...].astype(jnp.float32)
    gated = (local_ref[...] + carried) * (gate / (1.0 + jnp.exp(-gate)))
    gated_ref[...] = gated
    owner = lax.broadcasted_iota(jnp.int32, (TAIL_ROWS, width), 1) // HEAD_DIM
    heads = lax.broadcasted_iota(jnp.int32, (TAIL_ROWS, width), 0)
    sums = lax.dot_general(
        (owner == heads).astype(jnp.float32),
        gated * gated,
        (((1,), (1,)), ((), ())),
        precision=highest,
        preferred_element_type=jnp.float32,
    )
    squares_ref[0] = sums[:GROUPS, :]


def in_vmem(count):
    return [pl.BlockSpec(memory_space=pltpu.VMEM)] * count


def local_scan(inner, halo, taps, states, step, decay, skip, interpret=False):
    length, width = inner.shape
    return pl.pallas_call(
        local_scan_kernel,
        out_shape=(
            jax.ShapeDtypeStruct((length, width), jnp.float32),
            jax.ShapeDtypeStruct((1, STATE + 2 * TAIL_ROWS, width), jnp.bfloat16),
            jax.ShapeDtypeStruct((length, 128), jnp.float32),
        ),
        in_specs=in_vmem(7),
        out_specs=tuple(in_vmem(3)),
        scratch_shapes=[pltpu.VMEM((length + TAIL_ROWS, width), jnp.float32)],
        interpret=interpret,
        name="local_scan",
    )(inner, halo, taps, states, step, decay, skip)


def carry_in(position, messages, states, reach, local, gate, interpret=False):
    length, width = local.shape
    return pl.pallas_call(
        carry_kernel,
        out_shape=(
            jax.ShapeDtypeStruct((length, width), jnp.float32),
            jax.ShapeDtypeStruct((1, GROUPS, length), jnp.float32),
        ),
        in_specs=[pl.BlockSpec(memory_space=pltpu.SMEM)] + in_vmem(5),
        out_specs=tuple(in_vmem(2)),
        interpret=interpret,
        name="carry_in",
    )(position, messages, states, reach, local, gate)


def body(
    tokens,
    pre_gain,
    proj_inner,
    proj_gate,
    proj_states,
    proj_step,
    step_bias,
    log_rate,
    conv_inner,
    conv_states,
    skip_gain,
    norm_gain,
    proj_output,
):
    tokens_wide = tokens.astype(jnp.float32)
    normed = (
        tokens_wide
        * lax.rsqrt(jnp.mean(tokens_wide * tokens_wide, axis=1, keepdims=True) + epsilon)
        * pre_gain
    ).astype(jnp.bfloat16)
    count = lax.axis_size("tp")
    own_rows, features = tokens.shape
    row_count = count * own_rows
    fit = (2**20 // (2 * row_count) - 1) // 128 * 128
    cut = features - fit
    first_rows = lax.all_gather(normed[:, :cut], "tp", axis=0, tiled=True)
    last_rows = lax.all_gather(normed[:, cut:], "tp", axis=0, tiled=True)
    margin = TAPS - 1

    def project(weight):
        late = jnp.dot(last_rows, weight[cut:], preferred_element_type=jnp.float32)
        return late + jnp.dot(first_rows, weight[:cut], preferred_element_type=jnp.float32)

    def project_across(weight):
        dims = (((0,), (1,)), ((), ()))
        late = lax.dot_general(weight[cut:], last_rows, dims, preferred_element_type=jnp.float32)
        return late + lax.dot_general(
            weight[:cut], first_rows, dims, preferred_element_type=jnp.float32
        )

    state_proj = project_across(proj_states).astype(jnp.bfloat16)
    before_states = from_behind(state_proj[:, row_count - margin :], "seq", 1)
    inner_proj = project(proj_inner).astype(jnp.bfloat16)
    gate_proj = project(proj_gate).astype(jnp.bfloat16)
    step_size = jax.nn.softplus(project_across(proj_step) + step_bias[:, None])
    log_decay = -jnp.exp(log_rate)[:, None] * step_size
    before_inner = from_behind(inner_proj[row_count - margin :], "seq", 1)
    padded = jnp.concatenate((before_states, state_proj), axis=1).astype(jnp.float32)
    mixed_local = jnp.zeros(state_proj.shape, jnp.float32)
    for tap in range(TAPS):
        mixed_local = mixed_local + conv_states[tap][:, None] * padded[:, tap : tap + row_count]
    mixed_local = jax.nn.silu(mixed_local).astype(jnp.bfloat16)
    mixed_all = from_everyone(mixed_local, "tp").reshape(-1, row_count)
    skip_row = jnp.repeat(skip_gain, HEAD_DIM)[None]
    local, message, reach = local_scan(
        inner_proj, before_inner, conv_inner, mixed_all, step_size, log_decay, skip_row
    )
    messages = lax.all_gather(message, "seq", axis=0, tiled=True)
    position = lax.axis_index("seq").astype(jnp.int32).reshape(1)
    gated_out, head_squares = carry_in(position, messages, mixed_all, reach, local, gate_proj)
    every_square = from_everyone(head_squares[0], "tp")
    mean_square = jnp.sum(every_square, axis=0) / (GROUP_HEADS * HEAD_DIM)
    scale = jnp.repeat(lax.rsqrt(mean_square + epsilon).T, HEAD_DIM, axis=1)
    mixed_out = (gated_out * scale * norm_gain).astype(jnp.bfloat16)
    summed = lax.psum_scatter(
        jnp.dot(mixed_out, proj_output, preferred_element_type=jnp.float32).astype(jnp.bfloat16),
        "tp",
        scatter_dimension=0,
        tiled=True,
    ).astype(jnp.float32)
    return (tokens_wide + summed).astype(jnp.bfloat16)


def solution(mesh):
    placed = (
        P(("dp", "seq", "tp"), None),
        P(),
        P(None, "tp"),
        P(None, "tp"),
        P(None, "tp"),
        P(None, "tp"),
        P("tp"),
        P("tp"),
        P(None, "tp"),
        P(None, "tp"),
        P("tp"),
        P("tp"),
        P("tp", None),
    )
    return jax.shard_map(
        body, mesh=mesh, in_specs=placed, out_specs=P(("dp", "seq", "tp"), None), check_vma=False
    )
```

```python
import jax
import jax.numpy as jnp
from jax import lax
from jax.experimental import pallas as pl
from jax.experimental.pallas import tpu as pltpu
from jax.sharding import PartitionSpec as P

HEAD_DIM = 64
STATE = 128
GROUP_HEADS = 16
TAPS = 4
ORDER = (0, 4, 8, 12, 1, 5, 9, 13, 2, 6, 10, 14, 15, 3, 7, 11)
TAIL_ROWS = 8
GROUPS = 4


epsilon = 1e-05
highest = lax.Precision.HIGHEST


def from_behind(value, axis, steps):
    count = lax.axis_size(axis)
    initial, last = (max(0, -steps), min(count, count - steps))
    return lax.ppermute(value, axis, [(source, source + steps) for source in range(initial, last)])


def from_everyone(x, axis):
    copies = jnp.broadcast_to(x, (lax.axis_size(axis), *x.shape))
    return lax.all_to_all(copies, axis, split_axis=0, concat_axis=0, tiled=True)


def shifted(x, axis, steps):
    count = lax.axis_size(axis)
    return lax.ppermute(x, axis, [(k, (k + steps) % count) for k in range(count)])


def tree_gather(x, axis):
    opposite = shifted(x, axis, 8)
    behind = shifted(x, axis, 4)
    ahead = shifted(x, axis, -4)
    bundle = jnp.concatenate((x, ahead, opposite, behind), axis=0)
    rows = x.shape[0]
    half = x.shape[1] // 2
    below = shifted(bundle, axis, 1)
    above = shifted(bundle, axis, -1)
    left = shifted(bundle[:, :half], axis, 2)
    right = shifted(bundle[:, half:], axis, -2)
    left = jnp.concatenate((left[rows:], left[:rows]), axis=0)
    return bundle, above, jnp.concatenate((left, right), axis=1), below


def tree_scatter(rows_of, weight, axis):
    quarter = rows_of.shape[0] // 4
    piece = quarter // 4
    half = weight.shape[1] // 2
    own, above, second, below = (rows_of[k * quarter : (k + 1) * quarter] for k in range(4))
    turned = jnp.concatenate((second[3 * piece :], second[: 3 * piece]), axis=0)

    def sent(rows, columns, steps):
        part = jnp.dot(rows, columns, preferred_element_type=jnp.float32)
        return shifted(part.astype(jnp.bfloat16), axis, steps).astype(jnp.float32)

    rising = sent(above, weight, 1)
    falling = sent(below, weight, -1)
    left = sent(turned, weight[:, :half], -2)
    right = sent(second, weight[:, half:], 2)
    total = jnp.dot(own, weight, preferred_element_type=jnp.float32)
    total = total + rising + falling + jnp.concatenate((left, right), axis=1)
    passed = total[piece:].astype(jnp.bfloat16)
    opposite = shifted(passed[piece : 2 * piece], axis, 8)
    ahead = shifted(passed[:piece], axis, 4)
    behind = shifted(passed[2 * piece :], axis, -4)
    return (
        total[:piece]
        + opposite.astype(jnp.float32)
        + ahead.astype(jnp.float32)
        + behind.astype(jnp.float32)
    )


def placement(axis, piece):
    count = lax.axis_size(axis)
    size = count * piece
    slot = jnp.arange(size)
    source = (jnp.array(ORDER, jnp.int32)[slot // piece] + lax.axis_index(axis)) % count
    row = source * piece + slot % piece
    return (row[:, None] == jnp.arange(size)[None, :]).astype(jnp.bfloat16)


def split_dot(exact, wide, dims, exact_first):
    upper = wide.astype(jnp.bfloat16)
    lower = (wide - upper.astype(jnp.float32)).astype(jnp.bfloat16)

    def product(part):
        pair = (exact, part) if exact_first else (part, exact)
        return lax.dot_general(*pair, (dims, ((), ())), preferred_element_type=jnp.float32)

    return product(upper) + product(lower)


def head_lanes(columns, width):
    rows = columns.shape[0]
    return jnp.concatenate(
        [jnp.broadcast_to(columns[:, h : h + 1], (rows, width)) for h in range(GROUPS)], axis=1
    )


def local_scan_kernel(
    inner_ref, halo_ref, taps_ref, states_ref, step_ref, decay_ref, skip_ref,
    local_ref, message_ref, reach_ref, padded,
):
    length = inner_ref.shape[0]
    margin = TAPS - 1
    padded[TAIL_ROWS - margin : TAIL_ROWS, :] = halo_ref[...].astype(jnp.float32)
    padded[TAIL_ROWS:, :] = inner_ref[...].astype(jnp.float32)
    conv = jnp.zeros(inner_ref.shape, jnp.float32)
    for tap in range(TAPS):
        start = TAIL_ROWS - margin + tap
        conv = conv + taps_ref[tap : tap + 1, :] * padded[start : start + length, :]
    mixed = (conv / (1.0 + jnp.exp(-conv))).astype(jnp.bfloat16)
    rows = lax.broadcasted_iota(jnp.int32, (length, length), 0)
    cols = lax.broadcasted_iota(jnp.int32, (length, length), 1)
    lower_mask = rows >= cols
    blank = jnp.zeros((128 - GROUPS, length), jnp.float32)
    step_rows = step_ref[...]
    reach_rows = jnp.dot(
        jnp.concatenate((decay_ref[...], blank), axis=0),
        (rows <= cols).astype(jnp.float32),
        precision=highest,
        preferred_element_type=jnp.float32,
    )
    reach = reach_rows.T
    step = jnp.concatenate((step_rows, blank), axis=0).T
    reach_ref[...] = reach
    final = reach[length - 1 :, :]
    tail = jnp.exp(final - reach) * step
    mixed_wide = mixed.astype(jnp.float32)
    scaled = mixed_wide * head_lanes(tail, HEAD_DIM)
    outs = []
    ends = []
    for g in range(GROUPS):
        low = g * HEAD_DIM
        in_states = states_ref[2 * g * STATE : (2 * g + 1) * STATE, :]
        out_states = states_ref[(2 * g + 1) * STATE : (2 * g + 2) * STATE, :]
        scores = lax.dot_general(
            out_states, in_states, (((0,), (0,)), ((), ())), preferred_element_type=jnp.float32
        )
        spread = jnp.where(lower_mask, reach[:, g : g + 1] - reach_rows[g : g + 1, :], 0.0)
        decay_table = jnp.where(lower_mask, jnp.exp(spread), 0.0)
        weights = scores * decay_table * step_rows[g : g + 1, :]
        outs.append(split_dot(mixed[:, low : low + HEAD_DIM], weights, ((1,), (0,)), False))
        ends.append(split_dot(in_states, scaled[:, low : low + HEAD_DIM], ((1,), (0,)), True))
    local_ref[...] = jnp.concatenate(outs, axis=1) + skip_ref[...] * mixed_wide
    message_ref[0, :STATE, :] = jnp.concatenate(ends, axis=1).astype(jnp.bfloat16)
    total = head_lanes(final, HEAD_DIM)
    upper = total.astype(jnp.bfloat16)
    lower = (total - upper.astype(jnp.float32)).astype(jnp.bfloat16)
    zeros = jnp.zeros((TAIL_ROWS - 1, total.shape[1]), jnp.bfloat16)
    message_ref[0, STATE : STATE + TAIL_ROWS, :] = jnp.concatenate((upper, zeros), axis=0)
    message_ref[0, STATE + TAIL_ROWS :, :] = jnp.concatenate((lower, zeros), axis=0)


def carry_kernel(
    position_ref, messages_ref, states_ref, reach_ref, local_ref, gate_ref, gated_ref, squares_ref
):
    position = position_ref[0]
    width = local_ref.shape[1]
    carry = jnp.zeros((STATE, width), jnp.float32)
    for k in range(messages_ref.shape[0] - 1):
        total = messages_ref[k, STATE : STATE + TAIL_ROWS, :].astype(jnp.float32)
        total = total + messages_ref[k, STATE + TAIL_ROWS :, :].astype(jnp.float32)
        moved = jnp.exp(total[:1, :]) * carry + messages_ref[k, :STATE, :].astype(jnp.float32)
        carry = jnp.where(k < position, moved, carry)
    outs = []
    for g in range(GROUPS):
        low = g * HEAD_DIM
        out_states = states_ref[(2 * g + 1) * STATE : (2 * g + 2) * STATE, :]
        outs.append(split_dot(out_states, carry[:, low : low + HEAD_DIM], ((0,), (0,)), True))
    carried = jnp.concatenate(outs, axis=1) * head_lanes(jnp.exp(reach_ref[...]), HEAD_DIM)
    gate = gate_ref[...].astype(jnp.float32)
    gated = (local_ref[...] + carried) * (gate / (1.0 + jnp.exp(-gate)))
    gated_ref[...] = gated
    owner = lax.broadcasted_iota(jnp.int32, (TAIL_ROWS, width), 1) // HEAD_DIM
    heads = lax.broadcasted_iota(jnp.int32, (TAIL_ROWS, width), 0)
    sums = lax.dot_general(
        (owner == heads).astype(jnp.float32),
        gated * gated,
        (((1,), (1,)), ((), ())),
        precision=highest,
        preferred_element_type=jnp.float32,
    )
    squares_ref[0] = sums[:GROUPS, :]


def in_vmem(count):
    return [pl.BlockSpec(memory_space=pltpu.VMEM)] * count


def local_scan(inner, halo, taps, states, step, decay, skip, interpret=False):
    length, width = inner.shape
    return pl.pallas_call(
        local_scan_kernel,
        out_shape=(
            jax.ShapeDtypeStruct((length, width), jnp.float32),
            jax.ShapeDtypeStruct((1, STATE + 2 * TAIL_ROWS, width), jnp.bfloat16),
            jax.ShapeDtypeStruct((length, 128), jnp.float32),
        ),
        in_specs=in_vmem(7),
        out_specs=tuple(in_vmem(3)),
        scratch_shapes=[pltpu.VMEM((length + TAIL_ROWS, width), jnp.float32)],
        interpret=interpret,
        name="local_scan",
    )(inner, halo, taps, states, step, decay, skip)


def carry_in(position, messages, states, reach, local, gate, interpret=False):
    length, width = local.shape
    return pl.pallas_call(
        carry_kernel,
        out_shape=(
            jax.ShapeDtypeStruct((length, width), jnp.float32),
            jax.ShapeDtypeStruct((1, GROUPS, length), jnp.float32),
        ),
        in_specs=[pl.BlockSpec(memory_space=pltpu.SMEM)] + in_vmem(5),
        out_specs=tuple(in_vmem(2)),
        interpret=interpret,
        name="carry_in",
    )(position, messages, states, reach, local, gate)


def body(
    tokens,
    pre_gain,
    proj_inner,
    proj_gate,
    proj_states,
    proj_step,
    step_bias,
    log_rate,
    conv_inner,
    conv_states,
    skip_gain,
    norm_gain,
    proj_output,
):
    tokens_wide = tokens.astype(jnp.float32)
    normed = (
        tokens_wide
        * lax.rsqrt(jnp.mean(tokens_wide * tokens_wide, axis=1, keepdims=True) + epsilon)
        * pre_gain
    ).astype(jnp.bfloat16)
    own_rows = tokens.shape[0]
    margin = TAPS - 1
    place = placement("tp", own_rows)
    row_count = place.shape[0]
    across = (((0,), (1,)), ((), ()))
    along = (((0,), (0,)), ((), ()))
    flat = (((1,), (0,)), ((), ()))
    pieces = tree_gather(normed, "tp")

    def product(left, right, dims, precision=None):
        return lax.dot_general(
            left, right, dims, precision=precision, preferred_element_type=jnp.float32
        )

    def project(weight):
        found = [product(rows, weight, flat).astype(jnp.bfloat16) for rows in pieces]
        return product(place, jnp.concatenate(found, axis=0), along).astype(jnp.bfloat16)

    def project_across(weight):
        return jnp.concatenate([product(weight, rows, across) for rows in pieces], axis=1)

    state_proj = product(project_across(proj_states).astype(jnp.bfloat16), place, flat)
    state_proj = state_proj.astype(jnp.bfloat16)
    before_states = from_behind(state_proj[:, row_count - margin :], "seq", 1)
    inner_proj = project(proj_inner)
    gate_proj = project(proj_gate)
    steps = product(project_across(proj_step), place.astype(jnp.float32), flat, highest)
    step_size = jax.nn.softplus(steps + step_bias[:, None])
    log_decay = -jnp.exp(log_rate)[:, None] * step_size
    before_inner = from_behind(inner_proj[row_count - margin :], "seq", 1)
    padded = jnp.concatenate((before_states, state_proj), axis=1).astype(jnp.float32)
    mixed_local = jnp.zeros(state_proj.shape, jnp.float32)
    for tap in range(TAPS):
        mixed_local = mixed_local + conv_states[tap][:, None] * padded[:, tap : tap + row_count]
    mixed_local = jax.nn.silu(mixed_local).astype(jnp.bfloat16)
    mixed_all = from_everyone(mixed_local, "tp").reshape(-1, row_count)
    skip_row = jnp.repeat(skip_gain, HEAD_DIM)[None]
    local, message, reach = local_scan(
        inner_proj, before_inner, conv_inner, mixed_all, step_size, log_decay, skip_row
    )
    messages = lax.all_gather(message, "seq", axis=0, tiled=True)
    position = lax.axis_index("seq").astype(jnp.int32).reshape(1)
    gated_out, head_squares = carry_in(position, messages, mixed_all, reach, local, gate_proj)
    every_square = from_everyone(head_squares[0], "tp")
    mean_square = jnp.sum(every_square, axis=0) / (GROUP_HEADS * HEAD_DIM)
    scale = jnp.repeat(lax.rsqrt(mean_square + epsilon).T, HEAD_DIM, axis=1)
    mixed_out = (gated_out * scale * norm_gain).astype(jnp.bfloat16)
    rows_of = product(place, mixed_out, flat).astype(jnp.bfloat16)
    summed = tree_scatter(rows_of, proj_output, "tp")
    return (tokens_wide + summed).astype(jnp.bfloat16)


def solution(mesh):
    placed = (
        P(("dp", "seq", "tp"), None),
        P(),
        P(None, "tp"),
        P(None, "tp"),
        P(None, "tp"),
        P(None, "tp"),
        P("tp"),
        P("tp"),
        P(None, "tp"),
        P(None, "tp"),
        P("tp"),
        P("tp"),
        P("tp", None),
    )
    return jax.shard_map(
        body, mesh=mesh, in_specs=placed, out_specs=P(("dp", "seq", "tp"), None), check_vma=False
    )
```

```python
import jax
import jax.numpy as jnp
from jax import lax
from jax.experimental import pallas as pl
from jax.experimental.pallas import tpu as pltpu
from jax.sharding import PartitionSpec as P

HEAD_DIM = 64
STATE = 128
GROUP_HEADS = 16
TAPS = 4
ORDER = (0, 4, 8, 12, 1, 5, 9, 13, 2, 6, 10, 14, 15, 3, 7, 11)
TAIL_ROWS = 8
GROUPS = 4


epsilon = 1e-05
highest = lax.Precision.HIGHEST


def from_behind(value, axis, steps):
    count = lax.axis_size(axis)
    initial, last = (max(0, -steps), min(count, count - steps))
    return lax.ppermute(value, axis, [(source, source + steps) for source in range(initial, last)])


def from_everyone(x, axis):
    copies = jnp.broadcast_to(x, (lax.axis_size(axis), *x.shape))
    return lax.all_to_all(copies, axis, split_axis=0, concat_axis=0, tiled=True)


def shifted(x, axis, steps):
    count = lax.axis_size(axis)
    return lax.ppermute(x, axis, [(k, (k + steps) % count) for k in range(count)])


def tree_gather(x, axis):
    opposite = shifted(x, axis, 8)
    behind = shifted(x, axis, 4)
    ahead = shifted(x, axis, -4)
    bundle = jnp.concatenate((x, ahead, opposite, behind), axis=0)
    rows = x.shape[0]
    half = x.shape[1] // 2
    below = shifted(bundle, axis, 1)
    above = shifted(bundle, axis, -1)
    left = shifted(bundle[:, :half], axis, 2)
    right = shifted(bundle[:, half:], axis, -2)
    left = jnp.concatenate((left[rows:], left[:rows]), axis=0)
    return bundle, above, jnp.concatenate((left, right), axis=1), below


def tree_scatter(rows_of, weight, axis):
    quarter = rows_of.shape[0] // 4
    piece = quarter // 4
    half = weight.shape[1] // 2
    own, above, second, below = (rows_of[k * quarter : (k + 1) * quarter] for k in range(4))
    turned = jnp.concatenate((second[3 * piece :], second[: 3 * piece]), axis=0)

    def sums(rows, columns):
        part = jnp.dot(rows, columns, preferred_element_type=jnp.float32)
        return part.astype(jnp.bfloat16)

    def sent(part, steps):
        return shifted(part, axis, steps).astype(jnp.float32)

    rising = sent(sums(above, weight), 1)
    falling = sent(sums(below, weight), -1)
    left = sent(sums(turned, weight[:, :half]), -2)
    last = sums(second, weight[:, half:])
    right = sent(last, 2)
    own = lax.optimization_barrier((own, last))[0]
    total = jnp.dot(own, weight, preferred_element_type=jnp.float32)
    total = total + rising + falling + jnp.concatenate((left, right), axis=1)
    passed = total[piece:].astype(jnp.bfloat16)
    opposite = shifted(passed[piece : 2 * piece], axis, 8)
    ahead = shifted(passed[:piece], axis, 4)
    behind = shifted(passed[2 * piece :], axis, -4)
    return (
        total[:piece]
        + opposite.astype(jnp.float32)
        + ahead.astype(jnp.float32)
        + behind.astype(jnp.float32)
    )


def placement(axis, piece):
    count = lax.axis_size(axis)
    size = count * piece
    slot = jnp.arange(size)
    source = (jnp.array(ORDER, jnp.int32)[slot // piece] + lax.axis_index(axis)) % count
    row = source * piece + slot % piece
    return (row[:, None] == jnp.arange(size)[None, :]).astype(jnp.bfloat16)


def split_dot(exact, wide, dims, exact_first):
    upper = wide.astype(jnp.bfloat16)
    lower = (wide - upper.astype(jnp.float32)).astype(jnp.bfloat16)

    def product(part):
        pair = (exact, part) if exact_first else (part, exact)
        return lax.dot_general(*pair, (dims, ((), ())), preferred_element_type=jnp.float32)

    return product(upper) + product(lower)


def head_lanes(columns, width):
    rows = columns.shape[0]
    return jnp.concatenate(
        [jnp.broadcast_to(columns[:, h : h + 1], (rows, width)) for h in range(GROUPS)], axis=1
    )


def local_scan_kernel(
    inner_ref, halo_ref, taps_ref, states_ref, step_ref, decay_ref, skip_ref,
    local_ref, message_ref, reach_ref, padded,
):
    length = inner_ref.shape[0]
    margin = TAPS - 1
    padded[TAIL_ROWS - margin : TAIL_ROWS, :] = halo_ref[...].astype(jnp.float32)
    padded[TAIL_ROWS:, :] = inner_ref[...].astype(jnp.float32)
    conv = jnp.zeros(inner_ref.shape, jnp.float32)
    for tap in range(TAPS):
        start = TAIL_ROWS - margin + tap
        conv = conv + taps_ref[tap : tap + 1, :] * padded[start : start + length, :]
    mixed = (conv / (1.0 + jnp.exp(-conv))).astype(jnp.bfloat16)
    rows = lax.broadcasted_iota(jnp.int32, (length, length), 0)
    cols = lax.broadcasted_iota(jnp.int32, (length, length), 1)
    lower_mask = rows >= cols
    blank = jnp.zeros((128 - GROUPS, length), jnp.float32)
    step_rows = step_ref[...]
    reach_rows = jnp.dot(
        jnp.concatenate((decay_ref[...], blank), axis=0),
        (rows <= cols).astype(jnp.float32),
        precision=highest,
        preferred_element_type=jnp.float32,
    )
    reach = reach_rows.T
    step = jnp.concatenate((step_rows, blank), axis=0).T
    reach_ref[...] = reach
    final = reach[length - 1 :, :]
    tail = jnp.exp(final - reach) * step
    mixed_wide = mixed.astype(jnp.float32)
    scaled = mixed_wide * head_lanes(tail, HEAD_DIM)
    outs = []
    ends = []
    for g in range(GROUPS):
        low = g * HEAD_DIM
        in_states = states_ref[2 * g * STATE : (2 * g + 1) * STATE, :]
        out_states = states_ref[(2 * g + 1) * STATE : (2 * g + 2) * STATE, :]
        scores = lax.dot_general(
            out_states, in_states, (((0,), (0,)), ((), ())), preferred_element_type=jnp.float32
        )
        spread = jnp.where(lower_mask, reach[:, g : g + 1] - reach_rows[g : g + 1, :], 0.0)
        decay_table = jnp.where(lower_mask, jnp.exp(spread), 0.0)
        weights = scores * decay_table * step_rows[g : g + 1, :]
        outs.append(split_dot(mixed[:, low : low + HEAD_DIM], weights, ((1,), (0,)), False))
        ends.append(split_dot(in_states, scaled[:, low : low + HEAD_DIM], ((1,), (0,)), True))
    local_ref[...] = jnp.concatenate(outs, axis=1) + skip_ref[...] * mixed_wide
    message_ref[0, :STATE, :] = jnp.concatenate(ends, axis=1).astype(jnp.bfloat16)
    total = head_lanes(final, HEAD_DIM)
    upper = total.astype(jnp.bfloat16)
    lower = (total - upper.astype(jnp.float32)).astype(jnp.bfloat16)
    zeros = jnp.zeros((TAIL_ROWS - 1, total.shape[1]), jnp.bfloat16)
    message_ref[0, STATE : STATE + TAIL_ROWS, :] = jnp.concatenate((upper, zeros), axis=0)
    message_ref[0, STATE + TAIL_ROWS :, :] = jnp.concatenate((lower, zeros), axis=0)


def carry_kernel(
    position_ref, messages_ref, states_ref, reach_ref, local_ref, gate_ref, gated_ref, squares_ref
):
    position = position_ref[0]
    width = local_ref.shape[1]
    carry = jnp.zeros((STATE, width), jnp.float32)
    for k in range(messages_ref.shape[0] - 1):
        total = messages_ref[k, STATE : STATE + TAIL_ROWS, :].astype(jnp.float32)
        total = total + messages_ref[k, STATE + TAIL_ROWS :, :].astype(jnp.float32)
        moved = jnp.exp(total[:1, :]) * carry + messages_ref[k, :STATE, :].astype(jnp.float32)
        carry = jnp.where(k < position, moved, carry)
    outs = []
    for g in range(GROUPS):
        low = g * HEAD_DIM
        out_states = states_ref[(2 * g + 1) * STATE : (2 * g + 2) * STATE, :]
        outs.append(split_dot(out_states, carry[:, low : low + HEAD_DIM], ((0,), (0,)), True))
    carried = jnp.concatenate(outs, axis=1) * head_lanes(jnp.exp(reach_ref[...]), HEAD_DIM)
    gate = gate_ref[...].astype(jnp.float32)
    gated = (local_ref[...] + carried) * (gate / (1.0 + jnp.exp(-gate)))
    gated_ref[...] = gated
    owner = lax.broadcasted_iota(jnp.int32, (TAIL_ROWS, width), 1) // HEAD_DIM
    heads = lax.broadcasted_iota(jnp.int32, (TAIL_ROWS, width), 0)
    sums = lax.dot_general(
        (owner == heads).astype(jnp.float32),
        gated * gated,
        (((1,), (1,)), ((), ())),
        precision=highest,
        preferred_element_type=jnp.float32,
    )
    squares_ref[0] = sums[:GROUPS, :]


def in_vmem(count):
    return [pl.BlockSpec(memory_space=pltpu.VMEM)] * count


def local_scan(inner, halo, taps, states, step, decay, skip, interpret=False):
    length, width = inner.shape
    return pl.pallas_call(
        local_scan_kernel,
        out_shape=(
            jax.ShapeDtypeStruct((length, width), jnp.float32),
            jax.ShapeDtypeStruct((1, STATE + 2 * TAIL_ROWS, width), jnp.bfloat16),
            jax.ShapeDtypeStruct((length, 128), jnp.float32),
        ),
        in_specs=in_vmem(7),
        out_specs=tuple(in_vmem(3)),
        scratch_shapes=[pltpu.VMEM((length + TAIL_ROWS, width), jnp.float32)],
        interpret=interpret,
        name="local_scan",
    )(inner, halo, taps, states, step, decay, skip)


def carry_in(position, messages, states, reach, local, gate, interpret=False):
    length, width = local.shape
    return pl.pallas_call(
        carry_kernel,
        out_shape=(
            jax.ShapeDtypeStruct((length, width), jnp.float32),
            jax.ShapeDtypeStruct((1, GROUPS, length), jnp.float32),
        ),
        in_specs=[pl.BlockSpec(memory_space=pltpu.SMEM)] + in_vmem(5),
        out_specs=tuple(in_vmem(2)),
        interpret=interpret,
        name="carry_in",
    )(position, messages, states, reach, local, gate)


def body(
    tokens,
    pre_gain,
    proj_inner,
    proj_gate,
    proj_states,
    proj_step,
    step_bias,
    log_rate,
    conv_inner,
    conv_states,
    skip_gain,
    norm_gain,
    proj_output,
):
    tokens_wide = tokens.astype(jnp.float32)
    normed = (
        tokens_wide
        * lax.rsqrt(jnp.mean(tokens_wide * tokens_wide, axis=1, keepdims=True) + epsilon)
        * pre_gain
    ).astype(jnp.bfloat16)
    own_rows = tokens.shape[0]
    margin = TAPS - 1
    place = placement("tp", own_rows)
    row_count = place.shape[0]
    across = (((0,), (1,)), ((), ()))
    along = (((0,), (0,)), ((), ()))
    flat = (((1,), (0,)), ((), ()))
    pieces = tree_gather(normed, "tp")

    def product(left, right, dims, precision=None):
        return lax.dot_general(
            left, right, dims, precision=precision, preferred_element_type=jnp.float32
        )

    def project(weight):
        found = [product(rows, weight, flat).astype(jnp.bfloat16) for rows in pieces]
        return product(place, jnp.concatenate(found, axis=0), along).astype(jnp.bfloat16)

    def project_across(weight):
        return jnp.concatenate([product(weight, rows, across) for rows in pieces], axis=1)

    state_proj = product(project_across(proj_states).astype(jnp.bfloat16), place, flat)
    state_proj = state_proj.astype(jnp.bfloat16)
    before_states = from_behind(state_proj[:, row_count - margin :], "seq", 1)
    inner_proj = project(proj_inner)
    gate_proj = project(proj_gate)
    steps = product(project_across(proj_step), place.astype(jnp.float32), flat, highest)
    step_size = jax.nn.softplus(steps + step_bias[:, None])
    log_decay = -jnp.exp(log_rate)[:, None] * step_size
    before_inner = from_behind(inner_proj[row_count - margin :], "seq", 1)
    padded = jnp.concatenate((before_states, state_proj), axis=1).astype(jnp.float32)
    mixed_local = jnp.zeros(state_proj.shape, jnp.float32)
    for tap in range(TAPS):
        mixed_local = mixed_local + conv_states[tap][:, None] * padded[:, tap : tap + row_count]
    mixed_local = jax.nn.silu(mixed_local).astype(jnp.bfloat16)
    mixed_all = from_everyone(mixed_local, "tp").reshape(-1, row_count)
    skip_row = jnp.repeat(skip_gain, HEAD_DIM)[None]
    local, message, reach = local_scan(
        inner_proj, before_inner, conv_inner, mixed_all, step_size, log_decay, skip_row
    )
    messages = lax.all_gather(message, "seq", axis=0, tiled=True)
    position = lax.axis_index("seq").astype(jnp.int32).reshape(1)
    gated_out, head_squares = carry_in(position, messages, mixed_all, reach, local, gate_proj)
    every_square = from_everyone(head_squares[0], "tp")
    mean_square = jnp.sum(every_square, axis=0) / (GROUP_HEADS * HEAD_DIM)
    scale = jnp.repeat(lax.rsqrt(mean_square + epsilon).T, HEAD_DIM, axis=1)
    mixed_out = (gated_out * scale * norm_gain).astype(jnp.bfloat16)
    rows_of = product(place, mixed_out, flat).astype(jnp.bfloat16)
    summed = tree_scatter(rows_of, proj_output, "tp")
    return (tokens_wide + summed).astype(jnp.bfloat16)


def solution(mesh):
    placed = (
        P(("dp", "seq", "tp"), None),
        P(),
        P(None, "tp"),
        P(None, "tp"),
        P(None, "tp"),
        P(None, "tp"),
        P("tp"),
        P("tp"),
        P(None, "tp"),
        P(None, "tp"),
        P("tp"),
        P("tp"),
        P("tp", None),
    )
    return jax.shard_map(
        body, mesh=mesh, in_specs=placed, out_specs=P(("dp", "seq", "tp"), None), check_vma=False
    )
```

```python
import jax
import jax.numpy as jnp
from jax import lax
from jax.experimental import pallas as pl
from jax.experimental.pallas import tpu as pltpu
from jax.sharding import PartitionSpec as P

HEAD_DIM = 64
STATE = 128
GROUP_HEADS = 16
TAPS = 4
ORDER = (0, 4, 8, 12, 1, 5, 9, 13, 2, 6, 10, 14, 15, 3, 7, 11)
TAIL_ROWS = 8
GROUPS = 4


epsilon = 1e-05
highest = lax.Precision.HIGHEST


def from_behind(value, axis, steps):
    count = lax.axis_size(axis)
    initial, last = (max(0, -steps), min(count, count - steps))
    return lax.ppermute(value, axis, [(source, source + steps) for source in range(initial, last)])


def from_everyone(x, axis):
    copies = jnp.broadcast_to(x, (lax.axis_size(axis), *x.shape))
    return lax.all_to_all(copies, axis, split_axis=0, concat_axis=0, tiled=True)


def shifted(x, axis, steps):
    count = lax.axis_size(axis)
    return lax.ppermute(x, axis, [(k, (k + steps) % count) for k in range(count)])


def tree_gather(x, axis):
    opposite = shifted(x, axis, 8)
    behind = shifted(x, axis, 4)
    ahead = shifted(x, axis, -4)
    bundle = jnp.concatenate((x, ahead, opposite, behind), axis=0)
    rows = x.shape[0]
    half = x.shape[1] // 2
    below = shifted(bundle, axis, 1)
    above = shifted(bundle, axis, -1)
    left = shifted(bundle[:, :half], axis, 2)
    right = shifted(bundle[:, half:], axis, -2)
    left = jnp.concatenate((left[rows:], left[:rows]), axis=0)
    return bundle, above, jnp.concatenate((left, right), axis=1), below


def tree_scatter(rows_of, weight, axis):
    quarter = rows_of.shape[0] // 4
    piece = quarter // 4
    half = weight.shape[1] // 2
    own, above, second, below = (rows_of[k * quarter : (k + 1) * quarter] for k in range(4))
    turned = jnp.concatenate((second[3 * piece :], second[: 3 * piece]), axis=0)

    def sums(rows, columns):
        part = jnp.dot(rows, columns, preferred_element_type=jnp.float32)
        return part.astype(jnp.bfloat16)

    def sent(part, steps):
        return shifted(part, axis, steps).astype(jnp.float32)

    rising = sent(sums(above, weight), 1)
    falling = sent(sums(below, weight), -1)
    left = sent(sums(turned, weight[:, :half]), -2)
    last = sums(second, weight[:, half:])
    right = sent(last, 2)
    own = lax.optimization_barrier((own, last))[0]
    total = jnp.dot(own, weight, preferred_element_type=jnp.float32)
    total = total + rising + falling + jnp.concatenate((left, right), axis=1)
    passed = total[piece:].astype(jnp.bfloat16)
    opposite = shifted(passed[piece : 2 * piece], axis, 8)
    ahead = shifted(passed[:piece], axis, 4)
    behind = shifted(passed[2 * piece :], axis, -4)
    return (
        total[:piece]
        + opposite.astype(jnp.float32)
        + ahead.astype(jnp.float32)
        + behind.astype(jnp.float32)
    )


def placement(axis, piece):
    count = lax.axis_size(axis)
    size = count * piece
    slot = jnp.arange(size)
    source = (jnp.array(ORDER, jnp.int32)[slot // piece] + lax.axis_index(axis)) % count
    row = source * piece + slot % piece
    return (row[:, None] == jnp.arange(size)[None, :]).astype(jnp.bfloat16)


def split_dot(exact, wide, dims, exact_first):
    upper = wide.astype(jnp.bfloat16)
    lower = (wide - upper.astype(jnp.float32)).astype(jnp.bfloat16)

    def product(part):
        pair = (exact, part) if exact_first else (part, exact)
        return lax.dot_general(*pair, (dims, ((), ())), preferred_element_type=jnp.float32)

    return product(upper) + product(lower)


def head_lanes(columns, width):
    rows = columns.shape[0]
    return jnp.concatenate(
        [jnp.broadcast_to(columns[:, h : h + 1], (rows, width)) for h in range(GROUPS)], axis=1
    )


def prepare_kernel(
    inner_ref, halo_ref, taps_ref, step_ref, decay_ref, gate_ref,
    mixed_ref, scaled_ref, table_ref, reach_ref, total_ref, gate_out_ref, padded,
):
    length, width = inner_ref.shape
    margin = TAPS - 1
    padded[TAIL_ROWS - margin : TAIL_ROWS, :] = halo_ref[...].astype(jnp.float32)
    padded[TAIL_ROWS:, :] = inner_ref[...].astype(jnp.float32)
    conv = jnp.zeros((length, width), jnp.float32)
    for tap in range(TAPS):
        start = TAIL_ROWS - margin + tap
        conv = conv + taps_ref[tap : tap + 1, :] * padded[start : start + length, :]
    mixed = (conv / (1.0 + jnp.exp(-conv))).astype(jnp.bfloat16)
    mixed_ref[...] = mixed
    rows = lax.broadcasted_iota(jnp.int32, (length, length), 0)
    cols = lax.broadcasted_iota(jnp.int32, (length, length), 1)
    lower_mask = rows >= cols
    blank = jnp.zeros((128 - GROUPS, length), jnp.float32)
    step_rows = step_ref[...]
    reach_rows = jnp.dot(
        jnp.concatenate((decay_ref[...], blank), axis=0),
        (rows <= cols).astype(jnp.float32),
        precision=highest,
        preferred_element_type=jnp.float32,
    )
    reach = reach_rows.T
    step = jnp.concatenate((step_rows, blank), axis=0).T
    final = reach[length - 1 :, :]
    tail = jnp.exp(final - reach) * step
    scaled_ref[...] = mixed.astype(jnp.float32) * head_lanes(tail, HEAD_DIM)
    reach_ref[...] = head_lanes(jnp.exp(reach), HEAD_DIM)
    for g in range(GROUPS):
        spread = jnp.where(lower_mask, reach[:, g : g + 1] - reach_rows[g : g + 1, :], 0.0)
        decay_table = jnp.where(lower_mask, jnp.exp(spread), 0.0)
        table_ref[g] = decay_table * step_rows[g : g + 1, :]
    total = head_lanes(final, HEAD_DIM)
    upper = total.astype(jnp.bfloat16)
    lower = (total - upper.astype(jnp.float32)).astype(jnp.bfloat16)
    zeros = jnp.zeros((TAIL_ROWS - 1, width), jnp.bfloat16)
    total_ref[...] = jnp.concatenate((upper, zeros, lower, zeros), axis=0)
    gate = gate_ref[...].astype(jnp.float32)
    gate_out_ref[...] = gate / (1.0 + jnp.exp(-gate))


def local_scan_kernel(
    mixed_ref, scaled_ref, table_ref, total_ref, skip_ref, states_ref, local_ref, message_ref
):
    outs = []
    ends = []
    for g in range(GROUPS):
        low = g * HEAD_DIM
        in_states = states_ref[2 * g * STATE : (2 * g + 1) * STATE, :]
        out_states = states_ref[(2 * g + 1) * STATE : (2 * g + 2) * STATE, :]
        scores = lax.dot_general(
            out_states, in_states, (((0,), (0,)), ((), ())), preferred_element_type=jnp.float32
        )
        weights = scores * table_ref[g]
        outs.append(split_dot(mixed_ref[:, low : low + HEAD_DIM], weights, ((1,), (0,)), False))
        ends.append(split_dot(in_states, scaled_ref[:, low : low + HEAD_DIM], ((1,), (0,)), True))
    mixed_wide = mixed_ref[...].astype(jnp.float32)
    local_ref[...] = jnp.concatenate(outs, axis=1) + skip_ref[...] * mixed_wide
    message_ref[:STATE, :] = jnp.concatenate(ends, axis=1).astype(jnp.bfloat16)
    message_ref[STATE:, :] = total_ref[...]


def carry_kernel(
    core_ref, near_ref, mid_ref, far_ref, partner_ref, states_ref, reach_ref, local_ref, gate_ref,
    gated_ref, squares_ref,
):
    core = core_ref[0]
    width = local_ref.shape[1]

    def moved(message, carry):
        total = message[STATE : STATE + TAIL_ROWS, :].astype(jnp.float32)
        total = total + message[STATE + TAIL_ROWS :, :].astype(jnp.float32)
        return jnp.exp(total[:1, :]) * carry + message[:STATE, :].astype(jnp.float32)

    carry = jnp.zeros((STATE, width), jnp.float32)
    for pair_ref in (far_ref, mid_ref, near_ref):
        own = pair_ref[0]
        other = pair_ref[1]
        first = jnp.where(core == 0, own, other)
        second = jnp.where(core == 0, other, own)
        carry = moved(second, moved(first, carry))
    carry = jnp.where(core == 1, moved(partner_ref[...], carry), carry)
    outs = []
    for g in range(GROUPS):
        low = g * HEAD_DIM
        out_states = states_ref[(2 * g + 1) * STATE : (2 * g + 2) * STATE, :]
        outs.append(split_dot(out_states, carry[:, low : low + HEAD_DIM], ((0,), (0,)), True))
    carried = jnp.concatenate(outs, axis=1) * reach_ref[...]
    gated = (local_ref[...] + carried) * gate_ref[...]
    gated_ref[...] = gated
    owner = lax.broadcasted_iota(jnp.int32, (TAIL_ROWS, width), 1) // HEAD_DIM
    heads = lax.broadcasted_iota(jnp.int32, (TAIL_ROWS, width), 0)
    sums = lax.dot_general(
        (owner == heads).astype(jnp.float32),
        gated * gated,
        (((1,), (1,)), ((), ())),
        precision=highest,
        preferred_element_type=jnp.float32,
    )
    squares_ref[...] = sums[:GROUPS, :]


def in_vmem(count):
    return [pl.BlockSpec(memory_space=pltpu.VMEM)] * count


def prepare(inner, halo, taps, step, decay, gate, interpret=False):
    length, width = inner.shape
    wide = jax.ShapeDtypeStruct((length, width), jnp.float32)
    return pl.pallas_call(
        prepare_kernel,
        out_shape=(
            jax.ShapeDtypeStruct((length, width), jnp.bfloat16),
            wide,
            jax.ShapeDtypeStruct((GROUPS, length, length), jnp.float32),
            wide,
            jax.ShapeDtypeStruct((2 * TAIL_ROWS, width), jnp.bfloat16),
            wide,
        ),
        in_specs=in_vmem(6),
        out_specs=tuple(in_vmem(6)),
        scratch_shapes=[pltpu.VMEM((length + TAIL_ROWS, width), jnp.float32)],
        interpret=interpret,
        name="prepare",
    )(inner, halo, taps, step, decay, gate)


def local_scan(mixed, scaled, table, total, skip, states, interpret=False):
    length, width = mixed.shape
    return pl.pallas_call(
        local_scan_kernel,
        out_shape=(
            jax.ShapeDtypeStruct((length, width), jnp.float32),
            jax.ShapeDtypeStruct((STATE + 2 * TAIL_ROWS, width), jnp.bfloat16),
        ),
        in_specs=in_vmem(6),
        out_specs=tuple(in_vmem(2)),
        interpret=interpret,
        name="local_scan",
    )(mixed, scaled, table, total, skip, states)


def carry_in(core, near, mid, far, partner, states, reach, local, gate, interpret=False):
    length, width = local.shape
    return pl.pallas_call(
        carry_kernel,
        out_shape=(
            jax.ShapeDtypeStruct((length, width), jnp.float32),
            jax.ShapeDtypeStruct((GROUPS, length), jnp.float32),
        ),
        in_specs=[pl.BlockSpec(memory_space=pltpu.SMEM)] + in_vmem(8),
        out_specs=tuple(in_vmem(2)),
        interpret=interpret,
        name="carry_in",
    )(core, near, mid, far, partner, states, reach, local, gate)


def body(
    tokens,
    pre_gain,
    proj_inner,
    proj_gate,
    proj_states,
    proj_step,
    step_bias,
    log_rate,
    conv_inner,
    conv_states,
    skip_gain,
    norm_gain,
    proj_output,
):
    tokens_wide = tokens.astype(jnp.float32)
    normed = (
        tokens_wide
        * lax.rsqrt(jnp.mean(tokens_wide * tokens_wide, axis=1, keepdims=True) + epsilon)
        * pre_gain
    ).astype(jnp.bfloat16)
    own_rows = tokens.shape[0]
    margin = TAPS - 1
    place = placement("tp", own_rows)
    row_count = place.shape[0]
    across = (((0,), (1,)), ((), ()))
    along = (((0,), (0,)), ((), ()))
    flat = (((1,), (0,)), ((), ()))
    pieces = tree_gather(normed, "tp")

    def product(left, right, dims, precision=None):
        return lax.dot_general(
            left, right, dims, precision=precision, preferred_element_type=jnp.float32
        )

    def project(weight):
        found = [product(rows, weight, flat).astype(jnp.bfloat16) for rows in pieces]
        return product(place, jnp.concatenate(found, axis=0), along).astype(jnp.bfloat16)

    def project_across(weight):
        return jnp.concatenate([product(weight, rows, across) for rows in pieces], axis=1)

    state_proj = product(project_across(proj_states).astype(jnp.bfloat16), place, flat)
    state_proj = state_proj.astype(jnp.bfloat16)
    before_states = from_behind(state_proj[:, row_count - margin :], "seq", 1)
    inner_proj = project(proj_inner)
    gate_proj = project(proj_gate)
    steps = product(project_across(proj_step), place.astype(jnp.float32), flat, highest)
    step_size = jax.nn.softplus(steps + step_bias[:, None])
    log_decay = -jnp.exp(log_rate)[:, None] * step_size
    before_inner = from_behind(inner_proj[row_count - margin :], "seq", 1)
    padded = jnp.concatenate((before_states, state_proj), axis=1).astype(jnp.float32)
    mixed_local = jnp.zeros(state_proj.shape, jnp.float32)
    for tap in range(TAPS):
        mixed_local = mixed_local + conv_states[tap][:, None] * padded[:, tap : tap + row_count]
    mixed_local = jax.nn.silu(mixed_local).astype(jnp.bfloat16)
    mixed_all = from_everyone(mixed_local, "tp").reshape(-1, row_count)
    skip_row = jnp.repeat(skip_gain, HEAD_DIM)[None]
    mixed, scaled, table, reach, total, gate = prepare(
        inner_proj, before_inner, conv_inner, step_size, log_decay, gate_proj
    )
    local, message = local_scan(mixed, scaled, table, total, skip_row, mixed_all)
    shards = lax.axis_size("seq")
    partner = lax.ppermute(message, "seq", [(k, k ^ 1) for k in range(shards)])
    pair = jnp.stack((message, partner))
    far, mid, near = (from_behind(pair, "seq", steps) for steps in (6, 4, 2))
    core = (lax.axis_index("seq") % 2).astype(jnp.int32).reshape(1)
    gated_out, head_squares = carry_in(
        core, near, mid, far, partner, mixed_all, reach, local, gate
    )
    every_square = from_everyone(head_squares, "tp")
    mean_square = jnp.sum(every_square, axis=0) / (GROUP_HEADS * HEAD_DIM)
    scale = jnp.repeat(lax.rsqrt(mean_square + epsilon).T, HEAD_DIM, axis=1)
    mixed_out = (gated_out * scale * norm_gain).astype(jnp.bfloat16)
    rows_of = product(place, mixed_out, flat).astype(jnp.bfloat16)
    summed = tree_scatter(rows_of, proj_output, "tp")
    return (tokens_wide + summed).astype(jnp.bfloat16)


def solution(mesh):
    placed = (
        P(("dp", "seq", "tp"), None),
        P(),
        P(None, "tp"),
        P(None, "tp"),
        P(None, "tp"),
        P(None, "tp"),
        P("tp"),
        P("tp"),
        P(None, "tp"),
        P(None, "tp"),
        P("tp"),
        P("tp"),
        P("tp", None),
    )
    return jax.shard_map(
        body, mesh=mesh, in_specs=placed, out_specs=P(("dp", "seq", "tp"), None), check_vma=False
    )
```

```python
import jax
import jax.numpy as jnp
from jax import lax
from jax.experimental import pallas as pl
from jax.experimental.pallas import tpu as pltpu
from jax.sharding import PartitionSpec as P

HEAD_DIM = 64
STATE = 128
GROUP_HEADS = 16
TAPS = 4
VMEM_GRANT = 16 * 2**20
ORDER = (0, 4, 8, 12, 1, 5, 9, 13, 2, 6, 10, 14, 15, 3, 7, 11)
TAIL_ROWS = 8
GROUPS = 4


epsilon = 1e-05
highest = lax.Precision.HIGHEST


def from_behind(value, axis, steps):
    count = lax.axis_size(axis)
    initial, last = (max(0, -steps), min(count, count - steps))
    return lax.ppermute(value, axis, [(source, source + steps) for source in range(initial, last)])


def from_everyone(x, axis):
    copies = jnp.broadcast_to(x, (lax.axis_size(axis), *x.shape))
    return lax.all_to_all(copies, axis, split_axis=0, concat_axis=0, tiled=True)


def shifted(x, axis, steps):
    count = lax.axis_size(axis)
    return lax.ppermute(x, axis, [(k, (k + steps) % count) for k in range(count)])


def tree_gather(x, axis):
    opposite = shifted(x, axis, 8)
    behind = shifted(x, axis, 4)
    ahead = shifted(x, axis, -4)
    bundle = jnp.concatenate((x, ahead, opposite, behind), axis=0)
    rows = x.shape[0]
    half = x.shape[1] // 2
    below = shifted(bundle, axis, 1)
    above = shifted(bundle, axis, -1)
    left = shifted(bundle[:, :half], axis, 2)
    right = shifted(bundle[:, half:], axis, -2)
    left = jnp.concatenate((left[rows:], left[:rows]), axis=0)
    return bundle, above, jnp.concatenate((left, right), axis=1), below


def tree_scatter(rows_of, weight, axis):
    quarter = rows_of.shape[0] // 4
    piece = quarter // 4
    half = weight.shape[1] // 2
    own, above, second, below = (rows_of[k * quarter : (k + 1) * quarter] for k in range(4))
    turned = jnp.concatenate((second[3 * piece :], second[: 3 * piece]), axis=0)

    def sums(rows, columns):
        part = jnp.dot(rows, columns, preferred_element_type=jnp.float32)
        return part.astype(jnp.bfloat16)

    def sent(part, steps):
        return shifted(part, axis, steps).astype(jnp.float32)

    rising = sent(sums(above, weight), 1)
    falling = sent(sums(below, weight), -1)
    left = sent(sums(turned, weight[:, :half]), -2)
    last = sums(second, weight[:, half:])
    right = sent(last, 2)
    own = lax.optimization_barrier((own, last))[0]
    total = jnp.dot(own, weight, preferred_element_type=jnp.float32)
    total = total + rising + falling + jnp.concatenate((left, right), axis=1)
    passed = total[piece:].astype(jnp.bfloat16)
    opposite = shifted(passed[piece : 2 * piece], axis, 8)
    ahead = shifted(passed[:piece], axis, 4)
    behind = shifted(passed[2 * piece :], axis, -4)
    return (
        total[:piece]
        + opposite.astype(jnp.float32)
        + ahead.astype(jnp.float32)
        + behind.astype(jnp.float32)
    )


def placement(axis, piece):
    count = lax.axis_size(axis)
    size = count * piece
    slot = jnp.arange(size)
    source = (jnp.array(ORDER, jnp.int32)[slot // piece] + lax.axis_index(axis)) % count
    row = source * piece + slot % piece
    return (row[:, None] == jnp.arange(size)[None, :]).astype(jnp.bfloat16)


def split_dot(exact, wide, dims, exact_first):
    upper = wide.astype(jnp.bfloat16)
    lower = (wide - upper.astype(jnp.float32)).astype(jnp.bfloat16)

    def product(part):
        pair = (exact, part) if exact_first else (part, exact)
        return lax.dot_general(*pair, (dims, ((), ())), preferred_element_type=jnp.float32)

    return product(upper) + product(lower)


def head_lanes(columns, width):
    rows = columns.shape[0]
    return jnp.concatenate(
        [jnp.broadcast_to(columns[:, h : h + 1], (rows, width)) for h in range(GROUPS)], axis=1
    )


def local_scan_kernel(
    inner_ref, halo_ref, taps_ref, states_ref, step_ref, decay_ref, skip_ref,
    local_ref, message_ref, reach_ref, padded,
):
    length = inner_ref.shape[0]
    margin = TAPS - 1
    padded[TAIL_ROWS - margin : TAIL_ROWS, :] = halo_ref[...].astype(jnp.float32)
    padded[TAIL_ROWS:, :] = inner_ref[...].astype(jnp.float32)
    conv = jnp.zeros(inner_ref.shape, jnp.float32)
    for tap in range(TAPS):
        start = TAIL_ROWS - margin + tap
        conv = conv + taps_ref[tap : tap + 1, :] * padded[start : start + length, :]
    mixed = (conv / (1.0 + jnp.exp(-conv))).astype(jnp.bfloat16)
    rows = lax.broadcasted_iota(jnp.int32, (length, length), 0)
    cols = lax.broadcasted_iota(jnp.int32, (length, length), 1)
    lower_mask = rows >= cols
    blank = jnp.zeros((128 - GROUPS, length), jnp.float32)
    step_rows = step_ref[...]
    reach_rows = jnp.dot(
        jnp.concatenate((decay_ref[...], blank), axis=0),
        (rows <= cols).astype(jnp.float32),
        precision=highest,
        preferred_element_type=jnp.float32,
    )
    reach = reach_rows.T
    step = jnp.concatenate((step_rows, blank), axis=0).T
    reach_ref[...] = reach
    final = reach[length - 1 :, :]
    tail = jnp.exp(final - reach) * step
    mixed_wide = mixed.astype(jnp.float32)
    scaled = mixed_wide * head_lanes(tail, HEAD_DIM)
    outs = []
    ends = []
    for g in range(GROUPS):
        low = g * HEAD_DIM
        in_states = states_ref[2 * g * STATE : (2 * g + 1) * STATE, :]
        out_states = states_ref[(2 * g + 1) * STATE : (2 * g + 2) * STATE, :]
        scores = lax.dot_general(
            out_states, in_states, (((0,), (0,)), ((), ())), preferred_element_type=jnp.float32
        )
        spread = jnp.where(lower_mask, reach[:, g : g + 1] - reach_rows[g : g + 1, :], 0.0)
        decay_table = jnp.where(lower_mask, jnp.exp(spread), 0.0)
        weights = scores * decay_table * step_rows[g : g + 1, :]
        outs.append(split_dot(mixed[:, low : low + HEAD_DIM], weights, ((1,), (0,)), False))
        ends.append(split_dot(in_states, scaled[:, low : low + HEAD_DIM], ((1,), (0,)), True))
    local_ref[...] = jnp.concatenate(outs, axis=1) + skip_ref[...] * mixed_wide
    message_ref[0, :STATE, :] = jnp.concatenate(ends, axis=1).astype(jnp.bfloat16)
    total = head_lanes(final, HEAD_DIM)
    upper = total.astype(jnp.bfloat16)
    lower = (total - upper.astype(jnp.float32)).astype(jnp.bfloat16)
    zeros = jnp.zeros((TAIL_ROWS - 1, total.shape[1]), jnp.bfloat16)
    message_ref[0, STATE : STATE + TAIL_ROWS, :] = jnp.concatenate((upper, zeros), axis=0)
    message_ref[0, STATE + TAIL_ROWS :, :] = jnp.concatenate((lower, zeros), axis=0)


def carry_kernel(
    position_ref, messages_ref, states_ref, reach_ref, local_ref, gate_ref, gated_ref, squares_ref
):
    position = position_ref[0]
    width = local_ref.shape[1]
    carry = jnp.zeros((STATE, width), jnp.float32)
    for k in range(messages_ref.shape[0] - 1):
        total = messages_ref[k, STATE : STATE + TAIL_ROWS, :].astype(jnp.float32)
        total = total + messages_ref[k, STATE + TAIL_ROWS :, :].astype(jnp.float32)
        moved = jnp.exp(total[:1, :]) * carry + messages_ref[k, :STATE, :].astype(jnp.float32)
        carry = jnp.where(k < position, moved, carry)
    outs = []
    for g in range(GROUPS):
        low = g * HEAD_DIM
        out_states = states_ref[(2 * g + 1) * STATE : (2 * g + 2) * STATE, :]
        outs.append(split_dot(out_states, carry[:, low : low + HEAD_DIM], ((0,), (0,)), True))
    carried = jnp.concatenate(outs, axis=1) * head_lanes(jnp.exp(reach_ref[...]), HEAD_DIM)
    gate = gate_ref[...].astype(jnp.float32)
    gated = (local_ref[...] + carried) * (gate / (1.0 + jnp.exp(-gate)))
    gated_ref[...] = gated
    owner = lax.broadcasted_iota(jnp.int32, (TAIL_ROWS, width), 1) // HEAD_DIM
    heads = lax.broadcasted_iota(jnp.int32, (TAIL_ROWS, width), 0)
    sums = lax.dot_general(
        (owner == heads).astype(jnp.float32),
        gated * gated,
        (((1,), (1,)), ((), ())),
        precision=highest,
        preferred_element_type=jnp.float32,
    )
    squares_ref[0] = sums[:GROUPS, :]


def in_vmem(count):
    return [pl.BlockSpec(memory_space=pltpu.VMEM)] * count


def local_scan(inner, halo, taps, states, step, decay, skip, interpret=False):
    length, width = inner.shape
    return pl.pallas_call(
        local_scan_kernel,
        out_shape=(
            jax.ShapeDtypeStruct((length, width), jnp.float32),
            jax.ShapeDtypeStruct((1, STATE + 2 * TAIL_ROWS, width), jnp.bfloat16),
            jax.ShapeDtypeStruct((length, 128), jnp.float32),
        ),
        in_specs=in_vmem(7),
        out_specs=tuple(in_vmem(3)),
        scratch_shapes=[pltpu.VMEM((length + TAIL_ROWS, width), jnp.float32)],
        compiler_params=pltpu.CompilerParams(vmem_limit_bytes=VMEM_GRANT),
        interpret=interpret,
        name="local_scan",
    )(inner, halo, taps, states, step, decay, skip)


def carry_in(position, messages, states, reach, local, gate, interpret=False):
    length, width = local.shape
    return pl.pallas_call(
        carry_kernel,
        out_shape=(
            jax.ShapeDtypeStruct((length, width), jnp.float32),
            jax.ShapeDtypeStruct((1, GROUPS, length), jnp.float32),
        ),
        in_specs=[pl.BlockSpec(memory_space=pltpu.SMEM)] + in_vmem(5),
        out_specs=tuple(in_vmem(2)),
        compiler_params=pltpu.CompilerParams(vmem_limit_bytes=VMEM_GRANT),
        interpret=interpret,
        name="carry_in",
    )(position, messages, states, reach, local, gate)


def body(
    tokens,
    pre_gain,
    proj_inner,
    proj_gate,
    proj_states,
    proj_step,
    step_bias,
    log_rate,
    conv_inner,
    conv_states,
    skip_gain,
    norm_gain,
    proj_output,
):
    tokens_wide = tokens.astype(jnp.float32)
    normed = (
        tokens_wide
        * lax.rsqrt(jnp.mean(tokens_wide * tokens_wide, axis=1, keepdims=True) + epsilon)
        * pre_gain
    ).astype(jnp.bfloat16)
    own_rows = tokens.shape[0]
    margin = TAPS - 1
    place = placement("tp", own_rows)
    row_count = place.shape[0]
    across = (((0,), (1,)), ((), ()))
    along = (((0,), (0,)), ((), ()))
    flat = (((1,), (0,)), ((), ()))
    pieces = tree_gather(normed, "tp")

    def product(left, right, dims, precision=None):
        return lax.dot_general(
            left, right, dims, precision=precision, preferred_element_type=jnp.float32
        )

    def project(weight):
        found = [product(rows, weight, flat).astype(jnp.bfloat16) for rows in pieces]
        return product(place, jnp.concatenate(found, axis=0), along).astype(jnp.bfloat16)

    def project_across(weight):
        return jnp.concatenate([product(weight, rows, across) for rows in pieces], axis=1)

    state_proj = product(project_across(proj_states).astype(jnp.bfloat16), place, flat)
    state_proj = state_proj.astype(jnp.bfloat16)
    before_states = from_behind(state_proj[:, row_count - margin :], "seq", 1)
    steps = product(project_across(proj_step), place.astype(jnp.float32), flat, highest)
    step_size = jax.nn.softplus(steps + step_bias[:, None])
    log_decay = -jnp.exp(log_rate)[:, None] * step_size
    padded = jnp.concatenate((before_states, state_proj), axis=1).astype(jnp.float32)
    mixed_local = jnp.zeros(state_proj.shape, jnp.float32)
    for tap in range(TAPS):
        mixed_local = mixed_local + conv_states[tap][:, None] * padded[:, tap : tap + row_count]
    mixed_local = jax.nn.silu(mixed_local).astype(jnp.bfloat16)
    held = lax.optimization_barrier((pieces[1:], mixed_local))[0]
    pieces = (pieces[0], *held)
    inner_proj = project(proj_inner)
    gate_proj = project(proj_gate)
    before_inner = from_behind(inner_proj[row_count - margin :], "seq", 1)
    mixed_all = from_everyone(mixed_local, "tp").reshape(-1, row_count)
    skip_row = jnp.repeat(skip_gain, HEAD_DIM)[None]
    local, message, reach = local_scan(
        inner_proj, before_inner, conv_inner, mixed_all, step_size, log_decay, skip_row
    )
    messages = lax.all_gather(message, "seq", axis=0, tiled=True)
    position = lax.axis_index("seq").astype(jnp.int32).reshape(1)
    gated_out, head_squares = carry_in(position, messages, mixed_all, reach, local, gate_proj)
    every_square = from_everyone(head_squares[0], "tp")
    mean_square = jnp.sum(every_square, axis=0) / (GROUP_HEADS * HEAD_DIM)
    scale = jnp.repeat(lax.rsqrt(mean_square + epsilon).T, HEAD_DIM, axis=1)
    mixed_out = (gated_out * scale * norm_gain).astype(jnp.bfloat16)
    rows_of = product(place, mixed_out, flat).astype(jnp.bfloat16)
    summed = tree_scatter(rows_of, proj_output, "tp")
    return (tokens_wide + summed).astype(jnp.bfloat16)


def solution(mesh):
    placed = (
        P(("dp", "seq", "tp"), None),
        P(),
        P(None, "tp"),
        P(None, "tp"),
        P(None, "tp"),
        P(None, "tp"),
        P("tp"),
        P("tp"),
        P(None, "tp"),
        P(None, "tp"),
        P("tp"),
        P("tp"),
        P("tp", None),
    )
    return jax.shard_map(
        body, mesh=mesh, in_specs=placed, out_specs=P(("dp", "seq", "tp"), None), check_vma=False
    )
```
